32 devices in a mesh: lat: 16 (over z, x, core), tm: 2 (over y).
Axes of the slice: x: 2, y: 2, z: 4, core: 2. Of those that a mesh axis runs over, the one named last changes fastest.
Arguments:
- fields: bfloat16 [512, 64, 1024], P('lat', 'tm'), may hold values from -16 to 16
Outputs:
- covariance: float32 [64, 64], P('tm')
The draws below stay inside these ranges and needn't reach their ends.
All inputs are finite; a program needn't handle non-finite values.
Results may differ from the reference program's by a relative error of at most 0.0003.
Values may be sent and summed in bfloat16 or wider, within the bound.
A program may use at most 64 MiB of HBM per device.

```python
import math
import jax
import jax.numpy as jnp
from jax import lax

NLON = 1024
NLAT = 512
TRUNC = 341
MSLOT = 384
DSLOT = 384
MONTHS = 64


def draw_fields(key, part):
    patterns_count = 8
    half_lon = NLON // 2
    waves = jnp.arange(half_lon).astype(jnp.int32)
    longitude = jnp.arange(NLON).astype(jnp.int32)
    phase = 2.0 * math.pi * (waves[:, None] * longitude[None, :] % NLON).astype(jnp.float32) / NLON
    redness = 1.0 / (1.0 + waves.astype(jnp.float32) / (NLON / 2.0))
    cos_amps = jax.random.normal(jax.random.fold_in(key, 1), (patterns_count * NLAT, half_lon), jnp.float32) * redness
    sin_amps = jax.random.normal(jax.random.fold_in(key, 2), (patterns_count * NLAT, half_lon), jnp.float32) * redness
    patterns = jnp.dot(cos_amps, jnp.cos(phase)) + jnp.dot(sin_amps, jnp.sin(phase))
    patterns = patterns / jnp.sqrt(jnp.mean(patterns * patterns) + 1e-06)
    patterns = patterns.reshape(patterns_count, NLAT, NLON)
    month_amps = jax.random.normal(jax.random.fold_in(key, 3), (MONTHS, patterns_count), jnp.float32) / math.sqrt(patterns_count)
    month_scale = 1.0 + 2.0 * jnp.arange(MONTHS).astype(jnp.float32) / max(MONTHS - 1, 1)
    shared = jnp.einsum('tk,kjl->jtl', month_amps, patterns)
    noise = 0.5 * jax.random.normal(jax.random.fold_in(key, 4), (NLAT, MONTHS, NLON), jnp.float32)
    values = month_scale[None, :, None] * (shared + noise)
    return jnp.clip(values, -16.0, 16.0).astype(jnp.bfloat16)


def setup_inputs(seed: int = 0) -> dict:
    key_of = jax.random.split(jax.random.key(seed), 2)
    fields = draw_fields(jax.random.fold_in(key_of[1], 71), 0)
    return dict(fields=fields)


def start_value(order, sine_lat):
    log_start = 0.5 * (math.log(0.5) + lax.lgamma(order + 1.5) - (0.5 * math.log(math.pi) - math.log(2.0)) - lax.lgamma(order + 1.0)) + order * jnp.log(sine_lat)
    taper = jnp.clip((log_start + 70.0) / 10.0, 0.0, 1.0)
    return jnp.exp(jnp.maximum(log_start, -80.0)) * taper

def step_factors(order, degree):
    top = jnp.sqrt((4.0 * degree * degree - 1.0) / (degree * degree - order * order))
    below = degree - 1.0
    back = jnp.sqrt(jnp.maximum(below * below - order * order, 0.0) / jnp.abs(4.0 * below * below - 1.0))
    return (top, top * back)

def legendre_column(order, cosine_lat, sine_lat):
    first = start_value(order, sine_lat)

    def advance(carry, offset):
        current, previous = carry
        top, mixed = step_factors(order, order + offset)
        following = top * cosine_lat * current - mixed * previous
        return ((following, current), following)
    offsets = jnp.arange(1, DSLOT).astype(jnp.float32)
    _, later = lax.scan(advance, (first, jnp.zeros_like(first)), offsets)
    return jnp.concatenate([first[None, :], later], axis=0)

def weighted_basis(order, cosine_lat, sine_lat, weight):
    values = legendre_column(order, cosine_lat, sine_lat)
    offsets = jnp.arange(DSLOT).astype(jnp.float32)
    keep = (order + offsets <= TRUNC).astype(jnp.float32)
    factor = jnp.where(order > 0, math.sqrt(2.0), 1.0)
    table = values * keep[:, None] * weight[None, :] * factor
    return table.T.astype(jnp.bfloat16)

def reference(fields):
    longitude = jnp.arange(NLON).astype(jnp.int32)
    waves = jnp.arange(MSLOT).astype(jnp.int32)
    phase = 2.0 * math.pi * (longitude[:, None] * waves[None, :] % NLON).astype(jnp.float32) / NLON
    keep = (waves <= TRUNC).astype(jnp.float32)
    table = jnp.stack([jnp.cos(phase), -jnp.sin(phase)], axis=-1) * keep[None, :, None] / math.sqrt(NLON)
    table = table.reshape(NLON, 2 * MSLOT).astype(jnp.bfloat16)

    def per_row(row_fields):
        return jnp.dot(row_fields, table, preferred_element_type=jnp.float32).astype(jnp.bfloat16)
    fourier = lax.map(per_row, fields)
    fourier = fourier.reshape(NLAT, MONTHS, MSLOT, 2).transpose(2, 0, 1, 3)
    theta = math.pi * (jnp.arange(NLAT).astype(jnp.float32) + 0.5) / NLAT
    cosine_lat = jnp.cos(theta)
    sine_lat = jnp.sin(theta)
    weight = math.pi * sine_lat / NLAT

    def accumulate(gram, inputs):
        order_index, block = inputs
        order = order_index.astype(jnp.float32)
        basis = weighted_basis(order, cosine_lat, sine_lat, weight)
        coefficients = jnp.dot(block.reshape(NLAT, MONTHS * 2).T, basis, preferred_element_type=jnp.float32)
        coefficients = coefficients.astype(jnp.bfloat16).reshape(MONTHS, 2 * DSLOT)
        gram = gram + jnp.dot(coefficients, coefficients.T, preferred_element_type=jnp.float32)
        return (gram, None)
    gram, _ = lax.scan(accumulate, jnp.zeros((MONTHS, MONTHS), jnp.float32), (jnp.arange(MSLOT).astype(jnp.int32), fourier))
    trace = jnp.sum(jnp.diagonal(gram))
    return MONTHS * gram / (trace + 1e-06)
```

```python
import functools
import math

import jax
import jax.numpy as jnp
import numpy as np
from jax import lax
from jax.experimental import pallas as pl
from jax.experimental.pallas import tpu as pltpu
from jax.sharding import PartitionSpec as P

TRUNC = 341
LANES = 128
HALF = 64
PIECE = 8
PHASES = 3
MESH = pl.DeviceIdType.MESH


def phase_bounds(slots):
    length = -(-slots // PHASES)
    bounds = [(low, min(low + length, slots)) for low in range(0, slots, length)]
    low, top = bounds.pop()
    if top - low > 1:
        bounds.append((low, top - 1))
    return bounds + [(top - 1, top)]


def rank_of(lat, tm, lat_devices, tm_devices):
    hemisphere = lat_devices // 2
    return ((lat % hemisphere) * tm_devices + tm) * 2 + lat // hemisphere


def ranks(lat_devices, tm_devices):
    device = np.arange(lat_devices * tm_devices)
    return rank_of(device // tm_devices, device % tm_devices, lat_devices, tm_devices)


def twiddle_table(rank, slots, lon_count):
    device_total = len(rank)
    longitude = np.arange(lon_count)
    parts = []
    for low, top in phase_bounds(slots):
        wave = (np.arange(low, top)[None, :] * device_total + rank[:, None]).reshape(-1, 1)
        phase = 2.0 * math.pi * ((wave * longitude) % lon_count) / lon_count
        active = (wave <= TRUNC) / math.sqrt(lon_count)
        parts += [np.cos(phase) * active, -np.sin(phase) * active]
    return np.concatenate(parts).astype(np.float32).astype(jnp.bfloat16)


def start_table(rank, slots, slot_rows):
    device_total = len(rank)
    table = np.zeros((device_total, slot_rows), np.float64)
    for device in range(device_total):
        for slot in range(slot_rows):
            order = min(slot, slots - 1) * device_total + int(rank[device])
            table[device, slot] = 0.5 * (
                math.log(0.5)
                + math.lgamma(order + 1.5)
                - math.lgamma(1.5)
                - math.lgamma(order + 1.0)
            )
    table = np.broadcast_to(table[:, :, None], (device_total, slot_rows, LANES))
    return table.astype(np.float32)


def needed_slots(lat_devices, device_total, slots, rows, bands):
    counts = []
    order = np.arange(slots * device_total)
    rise = np.array(
        [math.lgamma(m + 1.5) - math.lgamma(1.5) - math.lgamma(m + 1.0) for m in order]
    )
    for device in range(lat_devices):
        lat = device * rows + np.arange(rows)
        sine = np.sin(math.pi * (lat + 0.5) / (lat_devices * rows))
        start = 0.5 * (math.log(0.5) + rise[:, None]) + order[:, None] * np.log(sine)[None, :]
        used = (start > -70.5) & (order <= TRUNC)[:, None]
        used = used.reshape(slots, device_total, bands, -1).any(axis=(1, 3))
        counts.append(
            tuple(
                int(np.max(np.nonzero(used[:, band])[0])) + 1 if used[:, band].any() else 0
                for band in range(bands)
            )
        )
    runs = []
    for device, count in enumerate(counts):
        if runs and runs[-1][2] == count:
            runs[-1][1] = device + 1
        else:
            runs.append([device, device + 1, count])
    return tuple(tuple(run) for run in runs)


def lat_table(lat_total, share):
    lat = np.arange(lat_total).reshape(lat_total // share, share).T.reshape(-1)
    theta = math.pi * (lat + 0.5) / lat_total
    table = np.stack([np.cos(theta), np.log(np.sin(theta)), math.pi * np.sin(theta) / lat_total])
    return table.reshape(3, lat_total // LANES, LANES).astype(np.float32)


def kernel(
    dims,
    runs,
    x_hbm,
    table_hbm,
    start_hbm,
    lat_hbm,
    out_ref,
    x_ref,
    table_ref,
    start_ref,
    lat_ref,
    spread,
    outbox,
    inbox,
    legendre,
    gram_ref,
    local_gram,
    parts,
    own_sum,
    full,
    x_sem,
    table_sem,
    small_sem,
    send_sem,
    recv_sem,
    tail_sem,
):
    lat_devices, tm_devices, rows, months, lon_count, slots, slot_rows, depth = dims
    device_total = lat_devices * tm_devices
    share = HALF // months
    high = rows // share
    lat_total = lat_devices * rows
    lat_groups = lat_total // LANES
    month_total = months * tm_devices
    pieces = month_total // PIECE
    lat_me = lax.axis_index("lat")
    tm_me = lax.axis_index("tm")
    me = lat_me * tm_devices + tm_me
    rank_me = rank_of(lat_me, tm_me, lat_devices, tm_devices)

    phases = phase_bounds(slots)

    def each_peer(act):
        def row(lat):
            for tm in range(tm_devices):
                act(lat, tm)

        pl.loop(lat_me + 1, lat_devices)(row)
        pl.loop(0, lat_me)(row)
        for tm in range(tm_devices):

            @pl.when(tm_me != tm)
            def _():
                act(lat_me, tm)

    barrier = pltpu.get_barrier_semaphore()
    each_peer(
        lambda lat, tm: pl.semaphore_signal(
            barrier, inc=1, device_id=(lat, tm), device_id_type=MESH
        )
    )

    x_copy = pltpu.make_async_copy(x_hbm, x_ref, x_sem)
    x_copy.start()

    def table_copy(phase):
        low, top = phases[phase]
        span = pl.ds(2 * device_total * low, 2 * device_total * (top - low))
        return pltpu.make_async_copy(table_hbm.at[span], table_ref.at[span], table_sem.at[phase])

    for phase in range(len(phases)):
        table_copy(phase).start()

    start_copy = pltpu.make_async_copy(start_hbm.at[me], start_ref, small_sem.at[0])
    start_copy.start()
    lat_copy = pltpu.make_async_copy(lat_hbm, lat_ref, small_sem.at[1])
    lat_copy.start()

    bands = len(runs[0][2])
    band_rows = high // bands
    for first, last, counts in runs:
        for band, count in enumerate(counts):
            if count < slots:

                @pl.loop(first * tm_devices, last * tm_devices)
                def _(source):
                    for slot in range(count, slots):
                        inbox[source, slot * bands + band] = jnp.zeros(
                            (band_rows, LANES), jnp.bfloat16
                        )

    def pieces_of(phase, counts):
        low, top = phases[phase]
        found = []
        shared = min(min(counts), top)
        if shared > low:
            found.append((low * bands, (shared - low) * bands))
        for band, count in enumerate(counts):
            for slot in range(max(low, min(counts)), min(count, top)):
                found.append((slot * bands + band, 1))
        return found

    def blocks_of(phase, counts):
        return sum(length for first, length in pieces_of(phase, counts))

    def arriving(phase):
        return sum(
            (last - first) * tm_devices * blocks_of(phase, counts) for first, last, counts in runs
        )

    def holds(phase, lat, tm):
        low, top = phases[phase]
        rank = rank_of(lat, tm, lat_devices, tm_devices)
        return low * device_total + rank <= TRUNC

    def holders(phase):
        return min(TRUNC + 1 - phases[phase][0] * device_total, device_total)

    def wait_blocks(semaphore, count):
        if count:
            span = spread.at[pl.ds(0, count * band_rows // 2)]
            pltpu.make_async_copy(span, span, semaphore).wait()

    def each_class(act):
        for first, last, counts in runs:

            @pl.when((lat_me >= first) & (lat_me < last))
            def _():
                act(counts)

    def transform(phase):
        low, top = phases[phase]
        group_rows = device_total * (top - low)
        lower = lax.broadcasted_iota(jnp.int32, (group_rows, LANES), 1) < HALF
        table_copy(phase).wait()
        values = lax.dot_general(
            table_ref[2 * device_total * low : 2 * device_total * top],
            x_ref[...],
            (((1,), (1,)), ((), ())),
            preferred_element_type=jnp.float32,
        )
        for block in range(rows * months // LANES):
            cosine = values[:group_rows, block * LANES : (block + 1) * LANES]
            sine = values[group_rows:, block * LANES : (block + 1) * LANES]
            even = jnp.where(lower, cosine, pltpu.roll(sine, HALF, 1))
            odd = jnp.where(lower, pltpu.roll(cosine, HALF, 1), sine)
            spread[pl.ds(2 * block, group_rows, stride=high), :] = even
            spread[pl.ds(2 * block + 1, group_rows, stride=high), :] = odd
        packed = spread[: group_rows * high].astype(jnp.bfloat16)
        outbox[:, low * bands : top * bands] = packed.reshape(
            device_total, (top - low) * bands, band_rows, LANES
        )

    def exchange(phase, piece, lat, tm):
        span = pl.ds(*piece)
        return pltpu.make_async_remote_copy(
            src_ref=outbox.at[lat * tm_devices + tm, span],
            dst_ref=inbox.at[me, span],
            send_sem=send_sem.at[phase],
            recv_sem=recv_sem.at[phase],
            device_id=(lat, tm),
            device_id_type=MESH,
        )

    all_hold = [holders(phase) == device_total for phase in range(len(phases))]

    def send(phase):
        def send_class(counts):
            def send_to(lat, tm):
                def go():
                    for piece in pieces_of(phase, counts):
                        exchange(phase, piece, lat, tm).start()

                if all_hold[phase]:
                    go()
                else:
                    pl.when(holds(phase, lat, tm))(go)

            if blocks_of(phase, counts):
                each_peer(send_to)

        each_class(send_class)

    def wait_sent(phase):
        def wait_class(counts):
            length = blocks_of(phase, counts)
            if all_hold[phase]:
                wait_blocks(send_sem.at[phase], (device_total - 1) * length)
            elif length:
                held = holds(phase, lat_me, tm_me)
                pl.when(held)(
                    lambda: wait_blocks(send_sem.at[phase], (holders(phase) - 1) * length)
                )
                pl.when(jnp.logical_not(held))(
                    lambda: wait_blocks(send_sem.at[phase], holders(phase) * length)
                )

        each_class(wait_class)

    def wait_arrived(phase):
        each_class(
            lambda counts: wait_blocks(
                recv_sem.at[phase], arriving(phase) - blocks_of(phase, counts)
            )
        )

    with jax.named_scope("xwait"):
        x_copy.wait()
    for phase in range(len(phases)):
        with jax.named_scope(f"transform{phase}"):
            transform(phase)
        if phase == 0:
            with jax.named_scope("barrier"):
                pl.semaphore_wait(barrier, device_total - 1)
        with jax.named_scope(f"send{phase}"):
            send(phase)

    inbox[me] = outbox[me]

    start_copy.wait()
    lat_copy.wait()

    halves = slot_rows // 8
    sub = lax.broadcasted_iota(jnp.int32, (8, LANES), 0)
    slot_of = [sub + 8 * half for half in range(halves)]
    order_int = [slot * device_total + rank_me for slot in slot_of]
    order = [value.astype(jnp.float32) for value in order_int]
    cosine_lat = [jnp.broadcast_to(lat_ref[0, pl.ds(g, 1), :], (8, LANES)) for g in range(lat_groups)]
    current = []
    scale = []
    for half in range(halves):
        factor = jnp.where(order_int[half] > 0, math.sqrt(2.0), 1.0)
        for g in range(lat_groups):
            log_start = (
                start_ref[pl.ds(8 * half, 8), :]
                + order[half] * jnp.broadcast_to(lat_ref[1, pl.ds(g, 1), :], (8, LANES))
            )
            taper = jnp.clip((log_start + 70.0) / 10.0, 0.0, 1.0)
            current.append(jnp.exp(jnp.maximum(log_start, -80.0)) * taper)
            scale.append(factor * jnp.broadcast_to(lat_ref[2, pl.ds(g, 1), :], (8, LANES)))

    def store(offset, values):
        for half in range(halves):
            keep = (order_int[half] + offset <= TRUNC) & (slot_of[half] < slots)
            for g in range(lat_groups):
                index = half * lat_groups + g
                value = jnp.where(keep, values[index] * scale[index], 0.0)
                legendre[g, pl.ds(8 * half * depth + offset, 8, stride=depth), :] = value

    store(0, current)

    def advance(offset, carry):
        now, before, backs = carry
        real = lax.convert_element_type(offset, jnp.float32)
        following = []
        next_backs = []
        for half in range(halves):
            degree = order[half] + real
            ratio = (4.0 * degree * degree - 1.0) / (real * (order[half] + degree))
            top = jnp.sqrt(ratio)
            next_backs.append(1.0 / top)
            for g in range(lat_groups):
                index = half * lat_groups + g
                following.append(
                    top * (cosine_lat[g] * now[index] - backs[half] * before[index])
                )
        store(offset, following)
        return following, now, next_backs

    zero = jnp.zeros((8, LANES), jnp.float32)
    with jax.named_scope("legendre"):
        lax.fori_loop(
            1,
            depth,
            advance,
            (current, [zero] * len(current), [zero] * halves),
            unroll=7,
        )

    per_share = lat_groups // share
    width = tm_devices * LANES
    share_of = lax.broadcasted_iota(jnp.int32, (depth, width), 1) % HALF // months
    gram_ref[...] = jnp.zeros_like(gram_ref)

    def add_slot(slot):
        received = jnp.concatenate(
            [
                jnp.concatenate(
                    [
                        inbox[lat_device * tm_devices + tm, pl.ds(slot * bands, bands)].reshape(
                            high, LANES
                        )
                        for lat_device in range(lat_devices)
                    ],
                    axis=0,
                )
                for tm in range(tm_devices)
            ],
            axis=1,
        )
        first = pl.multiple_of(slot * depth, 8)
        merged = None
        for part in range(share):
            basis = jnp.concatenate(
                [
                    legendre[part * per_share + g, pl.ds(first, depth), :].astype(jnp.bfloat16)
                    for g in range(per_share)
                ],
                axis=1,
            )
            product = jnp.dot(basis, received, preferred_element_type=jnp.float32)
            merged = product if part == 0 else jnp.where(share_of == part, product, merged)
        total = merged
        for part in range(1, share):
            total = total + pltpu.roll(merged, width - part * months, 1)
        coefficients = jnp.where(share_of == 0, total, 0.0).astype(jnp.bfloat16)
        gram_ref[...] += lax.dot_general(
            coefficients,
            coefficients,
            (((0,), (0,)), ((), ())),
            preferred_element_type=jnp.float32,
        )

    def finish(phase):
        low, top = phases[phase]
        with jax.named_scope(f"recv{phase}"):
            wait_arrived(phase)
        with jax.named_scope(f"slots{phase}"):
            pl.loop(low, top)(add_slot)

    for phase in range(len(phases)):
        if all_hold[phase]:
            finish(phase)
        else:
            pl.when(holds(phase, lat_me, tm_me))(functools.partial(finish, phase))

    gram = None
    for part in range(2):
        across = jnp.concatenate(
            [
                gram_ref[pl.ds(tm * LANES + part * HALF, months), :]
                for tm in range(tm_devices)
            ],
            axis=0,
        )
        block = jnp.concatenate(
            [
                across[:, tm * LANES + part * HALF : tm * LANES + part * HALF + months]
                for tm in range(tm_devices)
            ],
            axis=1,
        )
        gram = block if gram is None else gram + block
    local_gram[...] = gram.reshape(pieces, PIECE, month_total)

    owner_lats = -(-pieces // tm_devices)
    lat_step = max(lat_devices // 2 // owner_lats, 1)
    first_lat = lat_devices // 4 + lat_step - 1

    def owner(piece):
        return (first_lat + (piece // tm_devices) * lat_step, piece % tm_devices)

    def mine(piece):
        lat, tm = owner(piece)
        return (lat == lat_me) & (tm == tm_me)

    def send_part(piece, source):
        return pltpu.make_async_remote_copy(
            src_ref=local_gram.at[piece],
            dst_ref=parts.at[source],
            send_sem=tail_sem.at[0],
            recv_sem=tail_sem.at[1],
            device_id=owner(piece),
            device_id_type=MESH,
        )

    def send_sum(piece, lat, tm):
        return pltpu.make_async_remote_copy(
            src_ref=own_sum,
            dst_ref=full.at[piece],
            send_sem=tail_sem.at[2],
            recv_sem=tail_sem.at[3],
            device_id=(lat, tm),
            device_id_type=MESH,
        )

    def not_mine(piece):
        return jnp.logical_not(mine(piece))

    owns_any = (
        (lat_me >= first_lat)
        & ((lat_me - first_lat) % lat_step == 0)
        & ((lat_me - first_lat) // lat_step * tm_devices + tm_me < pieces)
    )

    def wait_refs(index, ref):
        pltpu.make_async_copy(ref, ref, tail_sem.at[index]).wait()

    def wait_pieces(index, ref):
        pl.when(owns_any)(lambda: wait_refs(index, ref.at[pl.ds(0, pieces - 1)]))
        pl.when(jnp.logical_not(owns_any))(lambda: wait_refs(index, ref))

    @pl.loop(0, pieces)
    def _(piece):
        @pl.when(not_mine(piece))
        def _():
            send_part(piece, me).start()

    with jax.named_scope("waitsend"):
        for phase in range(len(phases)):
            wait_sent(phase)

    with jax.named_scope("owner"):

        @pl.loop(0, pieces)
        def _(piece):
            @pl.when(mine(piece))
            def _():
                parts[me] = local_gram[piece]
                wait_refs(1, parts.at[pl.ds(0, device_total - 1)])
                total = jnp.sum(parts[...], axis=0)
                own_sum[...] = total
                full[piece] = total
                each_peer(lambda lat, tm: send_sum(piece, lat, tm).start())

    with jax.named_scope("waitsum"):

        wait_pieces(3, full)

    with jax.named_scope("norm"):
        gram = full[...].reshape(month_total, month_total)
        on_diagonal = lax.broadcasted_iota(jnp.int32, gram.shape, 0) == lax.broadcasted_iota(
            jnp.int32, gram.shape, 1
        )
        trace = jnp.sum(jnp.where(on_diagonal, gram, 0.0))
        here = full[pl.ds(tm_me * (months // PIECE), months // PIECE)].reshape(months, month_total)
        out_ref[...] = month_total * here / (trace + 1e-06)

    with jax.named_scope("drain"):
        wait_pieces(0, local_gram)

        @pl.when(owns_any)
        def _():
            wait_refs(2, parts.at[pl.ds(0, device_total - 1)])


def solution(mesh):
    lat_devices = mesh.shape["lat"]
    tm_devices = mesh.shape["tm"]
    device_total = lat_devices * tm_devices
    slots = -(-(TRUNC + 1) // device_total)
    slot_rows = -(-slots // 8) * 8
    depth = -(-(TRUNC + 1) // 8) * 8

    def local(fields):
        rows, months, lon_count = fields.shape
        month_total = months * tm_devices
        lat_total = rows * lat_devices
        share = HALF // months
        high = rows // share
        pieces = month_total // PIECE
        width = tm_devices * LANES
        dims = (lat_devices, tm_devices, rows, months, lon_count, slots, slot_rows, depth)
        rank = ranks(lat_devices, tm_devices)
        table = jnp.asarray(twiddle_table(rank, slots, lon_count))
        starts = jnp.asarray(start_table(rank, slots, slot_rows))
        lats = jnp.asarray(lat_table(lat_total, share))
        bands = 2 if high % 16 == 0 else 1
        runs = needed_slots(lat_devices, device_total, slots, rows, bands)
        phases = phase_bounds(slots)
        longest = max(top - low for low, top in phases)
        hbm = pl.BlockSpec(memory_space=pl.ANY)
        vmem = pl.BlockSpec(memory_space=pltpu.VMEM)
        dma = pltpu.SemaphoreType.DMA
        return pl.pallas_call(
            functools.partial(kernel, dims, runs),
            out_shape=jax.ShapeDtypeStruct((months, month_total), jnp.float32),
            in_specs=[hbm, hbm, hbm, hbm],
            out_specs=vmem,
            scratch_shapes=[
                pltpu.VMEM((rows * months, lon_count), jnp.bfloat16),
                pltpu.VMEM(table.shape, jnp.bfloat16),
                pltpu.VMEM(starts.shape[1:], jnp.float32),
                pltpu.VMEM(lats.shape, jnp.float32),
                pltpu.VMEM((device_total * longest * high, LANES), jnp.float32),
                pltpu.VMEM((device_total, slots * bands, high // bands, LANES), jnp.bfloat16),
                pltpu.VMEM((device_total, slots * bands, high // bands, LANES), jnp.bfloat16),
                pltpu.VMEM((lat_total // LANES, slot_rows * depth, LANES), jnp.float32),
                pltpu.VMEM((width, width), jnp.float32),
                pltpu.VMEM((pieces, PIECE, month_total), jnp.float32),
                pltpu.VMEM((device_total, PIECE, month_total), jnp.float32),
                pltpu.VMEM((PIECE, month_total), jnp.float32),
                pltpu.VMEM((pieces, PIECE, month_total), jnp.float32),
                dma,
                dma((len(phases),)),
                dma((2,)),
                dma((len(phases),)),
                dma((len(phases),)),
                dma((4,)),
            ],
            compiler_params=pltpu.CompilerParams(
                collective_id=0, has_side_effects=True, vmem_limit_bytes=60 * 1024 * 1024
            ),
        )(fields.reshape(rows * months, lon_count), table, starts, lats)

    return jax.shard_map(
        local, mesh=mesh, in_specs=(P("lat", "tm", None),), out_specs=P("tm", None), check_vma=False
    )
```

```python
import functools
import math

import jax
import jax.numpy as jnp
import numpy as np
from jax import lax
from jax.experimental import pallas as pl
from jax.experimental.pallas import tpu as pltpu
from jax.sharding import PartitionSpec as P

TRUNC = 341
LANES = 128
HALF = 64
PIECE = 8
PHASES = 3
MESH = pl.DeviceIdType.MESH


def phase_bounds(slots):
    length = -(-slots // PHASES)
    return [(low, min(low + length, slots)) for low in range(0, slots, length)]


def rank_of(lat, tm, lat_devices, tm_devices):
    hemisphere = lat_devices // 2
    return ((lat % hemisphere) * tm_devices + tm) * 2 + lat // hemisphere


def ranks(lat_devices, tm_devices):
    device = np.arange(lat_devices * tm_devices)
    return rank_of(device // tm_devices, device % tm_devices, lat_devices, tm_devices)


def twiddle_table(rank, slots, lon_count):
    device_total = len(rank)
    longitude = np.arange(lon_count)
    parts = []
    for low, top in phase_bounds(slots):
        wave = (np.arange(low, top)[None, :] * device_total + rank[:, None]).reshape(-1, 1)
        phase = 2.0 * math.pi * ((wave * longitude) % lon_count) / lon_count
        active = (wave <= TRUNC) / math.sqrt(lon_count)
        parts += [np.cos(phase) * active, -np.sin(phase) * active]
    return np.concatenate(parts).astype(np.float32).astype(jnp.bfloat16)


def start_table(rank, slots, slot_rows):
    device_total = len(rank)
    table = np.zeros((device_total, slot_rows), np.float64)
    for device in range(device_total):
        for slot in range(slot_rows):
            order = min(slot, slots - 1) * device_total + int(rank[device])
            table[device, slot] = 0.5 * (
                math.log(0.5)
                + math.lgamma(order + 1.5)
                - math.lgamma(1.5)
                - math.lgamma(order + 1.0)
            )
    table = np.broadcast_to(table[:, :, None], (device_total, slot_rows, LANES))
    return table.astype(np.float32)


def needed_slots(lat_devices, device_total, slots, rows, bands):
    counts = []
    order = np.arange(slots * device_total)
    rise = np.array(
        [math.lgamma(m + 1.5) - math.lgamma(1.5) - math.lgamma(m + 1.0) for m in order]
    )
    for device in range(lat_devices):
        lat = device * rows + np.arange(rows)
        sine = np.sin(math.pi * (lat + 0.5) / (lat_devices * rows))
        start = 0.5 * (math.log(0.5) + rise[:, None]) + order[:, None] * np.log(sine)[None, :]
        used = (start > -70.5) & (order <= TRUNC)[:, None]
        used = used.reshape(slots, device_total, bands, -1).any(axis=(1, 3))
        counts.append(
            tuple(
                int(np.max(np.nonzero(used[:, band])[0])) + 1 if used[:, band].any() else 0
                for band in range(bands)
            )
        )
    runs = []
    for device, count in enumerate(counts):
        if runs and runs[-1][2] == count:
            runs[-1][1] = device + 1
        else:
            runs.append([device, device + 1, count])
    return tuple(tuple(run) for run in runs)


def lat_table(lat_total, share):
    lat = np.arange(lat_total).reshape(lat_total // share, share).T.reshape(-1)
    theta = math.pi * (lat + 0.5) / lat_total
    table = np.stack([np.cos(theta), np.log(np.sin(theta)), math.pi * np.sin(theta) / lat_total])
    return table.reshape(3, lat_total // LANES, LANES).astype(np.float32)


def kernel(
    dims,
    runs,
    x_hbm,
    table_hbm,
    start_hbm,
    lat_hbm,
    out_ref,
    x_ref,
    table_ref,
    start_ref,
    lat_ref,
    spread,
    outbox,
    inbox,
    legendre,
    gram_ref,
    local_gram,
    parts,
    own_sum,
    full,
    x_sem,
    table_sem,
    small_sem,
    send_sem,
    recv_sem,
    tail_sem,
):
    lat_devices, tm_devices, rows, months, lon_count, slots, slot_rows, depth = dims
    device_total = lat_devices * tm_devices
    share = HALF // months
    high = rows // share
    lat_total = lat_devices * rows
    lat_groups = lat_total // LANES
    month_total = months * tm_devices
    pieces = month_total // PIECE
    lat_me = lax.axis_index("lat")
    tm_me = lax.axis_index("tm")
    me = lat_me * tm_devices + tm_me
    rank_me = rank_of(lat_me, tm_me, lat_devices, tm_devices)

    phases = phase_bounds(slots)

    def each_peer(act):
        def row(lat):
            for tm in range(tm_devices):
                act(lat, tm)

        pl.loop(lat_me + 1, lat_devices)(row)
        pl.loop(0, lat_me)(row)
        for tm in range(tm_devices):

            @pl.when(tm_me != tm)
            def _():
                act(lat_me, tm)

    barrier = pltpu.get_barrier_semaphore()
    each_peer(
        lambda lat, tm: pl.semaphore_signal(
            barrier, inc=1, device_id=(lat, tm), device_id_type=MESH
        )
    )

    x_copy = pltpu.make_async_copy(x_hbm, x_ref, x_sem)
    x_copy.start()

    def table_copy(phase):
        low, top = phases[phase]
        span = pl.ds(2 * device_total * low, 2 * device_total * (top - low))
        return pltpu.make_async_copy(table_hbm.at[span], table_ref.at[span], table_sem.at[phase])

    for phase in range(len(phases)):
        table_copy(phase).start()

    start_copy = pltpu.make_async_copy(start_hbm.at[me], start_ref, small_sem.at[0])
    start_copy.start()
    lat_copy = pltpu.make_async_copy(lat_hbm, lat_ref, small_sem.at[1])
    lat_copy.start()

    bands = len(runs[0][2])
    band_rows = high // bands
    for first, last, counts in runs:
        for band, count in enumerate(counts):
            if count < slots:

                @pl.loop(first * tm_devices, last * tm_devices)
                def _(source):
                    for slot in range(count, slots):
                        inbox[source, slot * bands + band] = jnp.zeros(
                            (band_rows, LANES), jnp.bfloat16
                        )

    last_order = (slots - 1) * device_total
    last_holders = min(TRUNC + 1 - last_order, device_total)

    def holds_last(lat, tm):
        return last_order + rank_of(lat, tm, lat_devices, tm_devices) <= TRUNC

    def splits(phase):
        return phases[phase][1] == slots and last_holders < device_total

    if last_holders < device_total:

        @pl.when(jnp.logical_not(holds_last(lat_me, tm_me)))
        def _():
            inbox[:, (slots - 1) * bands :] = jnp.zeros(
                (device_total, bands, band_rows, LANES), jnp.bfloat16
            )

    def pieces_of(phase, counts, held):
        low, top = phases[phase]
        if not held:
            top = min(top, slots - 1)
        found = []
        shared = min(min(counts), top)
        if shared > low:
            found.append((low * bands, (shared - low) * bands))
        for band, count in enumerate(counts):
            for slot in range(max(low, min(counts)), min(count, top)):
                found.append((slot * bands + band, 1))
        return found

    def blocks_of(phase, counts, held):
        return sum(length for first, length in pieces_of(phase, counts, held))

    def leaving(phase, counts, held):
        kept = blocks_of(phase, counts, True) * last_holders
        rest = blocks_of(phase, counts, False) * (device_total - last_holders)
        return kept + rest - blocks_of(phase, counts, held)

    def arriving(phase, counts, held):
        total = sum(
            (last - first) * tm_devices * blocks_of(phase, counts, held)
            for first, last, counts in runs
        )
        return total - blocks_of(phase, counts, held)

    def each_case(phase, held, act):
        if splits(phase):
            pl.when(held)(lambda: act(True))
            pl.when(jnp.logical_not(held))(lambda: act(False))
        else:
            act(True)

    def wait_blocks(semaphore, count):
        if count:
            span = spread.at[pl.ds(0, count * band_rows // 2)]
            pltpu.make_async_copy(span, span, semaphore).wait()

    def each_class(act):
        for first, last, counts in runs:

            @pl.when((lat_me >= first) & (lat_me < last))
            def _():
                act(counts)

    def transform(phase):
        low, top = phases[phase]
        group_rows = device_total * (top - low)
        lower = lax.broadcasted_iota(jnp.int32, (group_rows, LANES), 1) < HALF
        table_copy(phase).wait()
        values = lax.dot_general(
            table_ref[2 * device_total * low : 2 * device_total * top],
            x_ref[...],
            (((1,), (1,)), ((), ())),
            preferred_element_type=jnp.float32,
        )
        for block in range(rows * months // LANES):
            cosine = values[:group_rows, block * LANES : (block + 1) * LANES]
            sine = values[group_rows:, block * LANES : (block + 1) * LANES]
            even = jnp.where(lower, cosine, pltpu.roll(sine, HALF, 1))
            odd = jnp.where(lower, pltpu.roll(cosine, HALF, 1), sine)
            spread[pl.ds(2 * block, group_rows, stride=high), :] = even
            spread[pl.ds(2 * block + 1, group_rows, stride=high), :] = odd
        packed = spread[: group_rows * high].astype(jnp.bfloat16)
        outbox[:, low * bands : top * bands] = packed.reshape(
            device_total, (top - low) * bands, band_rows, LANES
        )

    def exchange(phase, piece, lat, tm):
        span = pl.ds(*piece)
        return pltpu.make_async_remote_copy(
            src_ref=outbox.at[lat * tm_devices + tm, span],
            dst_ref=inbox.at[me, span],
            send_sem=send_sem.at[phase],
            recv_sem=recv_sem.at[phase],
            device_id=(lat, tm),
            device_id_type=MESH,
        )

    def send(phase):
        def send_class(counts):
            def send_to(lat, tm):
                def go(held):
                    for piece in pieces_of(phase, counts, held):
                        exchange(phase, piece, lat, tm).start()

                each_case(phase, holds_last(lat, tm), go)

            if pieces_of(phase, counts, True):
                each_peer(send_to)

        each_class(send_class)

    held_here = holds_last(lat_me, tm_me)

    def wait_moved(phase, semaphore, amount):
        each_class(
            lambda counts: each_case(
                phase,
                held_here,
                lambda held: wait_blocks(semaphore.at[phase], amount(phase, counts, held)),
            )
        )

    with jax.named_scope("xwait"):
        x_copy.wait()
    for phase in range(len(phases)):
        with jax.named_scope(f"transform{phase}"):
            transform(phase)
        if phase == 0:
            with jax.named_scope("barrier"):
                pl.semaphore_wait(barrier, device_total - 1)
        with jax.named_scope(f"send{phase}"):
            send(phase)

    inbox[me] = outbox[me]

    start_copy.wait()
    lat_copy.wait()

    halves = slot_rows // 8
    sub = lax.broadcasted_iota(jnp.int32, (8, LANES), 0)
    slot_of = [sub + 8 * half for half in range(halves)]
    order_int = [slot * device_total + rank_me for slot in slot_of]
    order = [value.astype(jnp.float32) for value in order_int]
    cosine_lat = [jnp.broadcast_to(lat_ref[0, pl.ds(g, 1), :], (8, LANES)) for g in range(lat_groups)]
    current = []
    scale = []
    for half in range(halves):
        factor = jnp.where(order_int[half] > 0, math.sqrt(2.0), 1.0)
        for g in range(lat_groups):
            log_start = (
                start_ref[pl.ds(8 * half, 8), :]
                + order[half] * jnp.broadcast_to(lat_ref[1, pl.ds(g, 1), :], (8, LANES))
            )
            taper = jnp.clip((log_start + 70.0) / 10.0, 0.0, 1.0)
            current.append(jnp.exp(jnp.maximum(log_start, -80.0)) * taper)
            scale.append(factor * jnp.broadcast_to(lat_ref[2, pl.ds(g, 1), :], (8, LANES)))

    def store(offset, values):
        for half in range(halves):
            keep = (order_int[half] + offset <= TRUNC) & (slot_of[half] < slots)
            for g in range(lat_groups):
                index = half * lat_groups + g
                value = jnp.where(keep, values[index] * scale[index], 0.0)
                legendre[g, pl.ds(8 * half * depth + offset, 8, stride=depth), :] = value

    store(0, current)

    def advance(offset, carry):
        now, before, backs = carry
        real = lax.convert_element_type(offset, jnp.float32)
        following = []
        next_backs = []
        for half in range(halves):
            degree = order[half] + real
            ratio = (4.0 * degree * degree - 1.0) / (real * (order[half] + degree))
            top = jnp.sqrt(ratio)
            next_backs.append(1.0 / top)
            for g in range(lat_groups):
                index = half * lat_groups + g
                following.append(
                    top * (cosine_lat[g] * now[index] - backs[half] * before[index])
                )
        store(offset, following)
        return following, now, next_backs

    zero = jnp.zeros((8, LANES), jnp.float32)
    with jax.named_scope("legendre"):
        lax.fori_loop(
            1,
            depth,
            advance,
            (current, [zero] * len(current), [zero] * halves),
            unroll=7,
        )

    per_share = lat_groups // share
    width = tm_devices * LANES

    def coefficients(slot, height):
        received = jnp.concatenate(
            [
                jnp.concatenate(
                    [
                        inbox[lat_device * tm_devices + tm, slot * bands : (slot + 1) * bands].reshape(
                            high, LANES
                        )
                        for lat_device in range(lat_devices)
                    ],
                    axis=0,
                )
                for tm in range(tm_devices)
            ],
            axis=1,
        )
        share_of = lax.broadcasted_iota(jnp.int32, (height, width), 1) % HALF // months
        first = slot * depth
        merged = None
        for part in range(share):
            basis = jnp.concatenate(
                [
                    legendre[part * per_share + g, first : first + height, :].astype(jnp.bfloat16)
                    for g in range(per_share)
                ],
                axis=1,
            )
            product = jnp.dot(basis, received, preferred_element_type=jnp.float32)
            merged = product if part == 0 else jnp.where(share_of == part, product, merged)
        total = merged
        for part in range(1, share):
            total = total + pltpu.roll(merged, width - part * months, 1)
        return jnp.where(share_of == 0, total, 0.0).astype(jnp.bfloat16)

    for phase, (low, top) in enumerate(phases):
        with jax.named_scope(f"recv{phase}"):
            wait_moved(phase, recv_sem, arriving)
        with jax.named_scope(f"slots{phase}"):
            heights = [
                min(-(-(TRUNC + 1 - slot * device_total) // 16) * 16, depth)
                for slot in range(low, top)
            ]
            values = jnp.concatenate(
                [coefficients(low + index, height) for index, height in enumerate(heights)],
                axis=0,
            )
            product = lax.dot_general(
                values, values, (((0,), (0,)), ((), ())), preferred_element_type=jnp.float32
            )
            gram_ref[...] = product if phase == 0 else gram_ref[...] + product

    gram = None
    for part in range(2):
        across = jnp.concatenate(
            [
                gram_ref[pl.ds(tm * LANES + part * HALF, months), :]
                for tm in range(tm_devices)
            ],
            axis=0,
        )
        block = jnp.concatenate(
            [
                across[:, tm * LANES + part * HALF : tm * LANES + part * HALF + months]
                for tm in range(tm_devices)
            ],
            axis=1,
        )
        gram = block if gram is None else gram + block
    local_gram[...] = gram.reshape(pieces, PIECE, month_total)

    owner_lats = -(-pieces // tm_devices)
    lat_step = max(lat_devices // 2 // owner_lats, 1)
    first_lat = lat_devices // 4 + lat_step - 1

    def owner(piece):
        return (first_lat + (piece // tm_devices) * lat_step, piece % tm_devices)

    def mine(piece):
        lat, tm = owner(piece)
        return (lat == lat_me) & (tm == tm_me)

    def send_part(piece, source):
        return pltpu.make_async_remote_copy(
            src_ref=local_gram.at[piece],
            dst_ref=parts.at[source],
            send_sem=tail_sem.at[0],
            recv_sem=tail_sem.at[1],
            device_id=owner(piece),
            device_id_type=MESH,
        )

    def send_sum(piece, lat, tm):
        return pltpu.make_async_remote_copy(
            src_ref=own_sum,
            dst_ref=full.at[piece],
            send_sem=tail_sem.at[2],
            recv_sem=tail_sem.at[3],
            device_id=(lat, tm),
            device_id_type=MESH,
        )

    def not_mine(piece):
        return jnp.logical_not(mine(piece))

    owns_any = (
        (lat_me >= first_lat)
        & ((lat_me - first_lat) % lat_step == 0)
        & ((lat_me - first_lat) // lat_step * tm_devices + tm_me < pieces)
    )

    def wait_refs(index, ref):
        pltpu.make_async_copy(ref, ref, tail_sem.at[index]).wait()

    def wait_pieces(index, ref):
        pl.when(owns_any)(lambda: wait_refs(index, ref.at[pl.ds(0, pieces - 1)]))
        pl.when(jnp.logical_not(owns_any))(lambda: wait_refs(index, ref))

    @pl.loop(0, pieces)
    def _(piece):
        @pl.when(not_mine(piece))
        def _():
            send_part(piece, me).start()

    with jax.named_scope("waitsend"):
        for phase in range(len(phases)):
            wait_moved(phase, send_sem, leaving)

    with jax.named_scope("owner"):

        @pl.loop(0, pieces)
        def _(piece):
            @pl.when(mine(piece))
            def _():
                parts[me] = local_gram[piece]
                wait_refs(1, parts.at[pl.ds(0, device_total - 1)])
                total = jnp.sum(parts[...], axis=0)
                own_sum[...] = total
                full[piece] = total
                each_peer(lambda lat, tm: send_sum(piece, lat, tm).start())

    with jax.named_scope("waitsum"):

        wait_pieces(3, full)

    with jax.named_scope("norm"):
        gram = full[...].reshape(month_total, month_total)
        on_diagonal = lax.broadcasted_iota(jnp.int32, gram.shape, 0) == lax.broadcasted_iota(
            jnp.int32, gram.shape, 1
        )
        trace = jnp.sum(jnp.where(on_diagonal, gram, 0.0))
        here = full[pl.ds(tm_me * (months // PIECE), months // PIECE)].reshape(months, month_total)
        out_ref[...] = month_total * here / (trace + 1e-06)

    with jax.named_scope("drain"):
        wait_pieces(0, local_gram)

        @pl.when(owns_any)
        def _():
            wait_refs(2, parts.at[pl.ds(0, device_total - 1)])


def solution(mesh):
    lat_devices = mesh.shape["lat"]
    tm_devices = mesh.shape["tm"]
    device_total = lat_devices * tm_devices
    slots = -(-(TRUNC + 1) // device_total)
    slot_rows = -(-slots // 8) * 8
    depth = -(-(TRUNC + 1) // 8) * 8

    def local(fields):
        rows, months, lon_count = fields.shape
        month_total = months * tm_devices
        lat_total = rows * lat_devices
        share = HALF // months
        high = rows // share
        pieces = month_total // PIECE
        width = tm_devices * LANES
        dims = (lat_devices, tm_devices, rows, months, lon_count, slots, slot_rows, depth)
        rank = ranks(lat_devices, tm_devices)
        table = jnp.asarray(twiddle_table(rank, slots, lon_count))
        starts = jnp.asarray(start_table(rank, slots, slot_rows))
        lats = jnp.asarray(lat_table(lat_total, share))
        bands = 2 if high % 16 == 0 else 1
        runs = needed_slots(lat_devices, device_total, slots, rows, bands)
        phases = phase_bounds(slots)
        longest = max(top - low for low, top in phases)
        hbm = pl.BlockSpec(memory_space=pl.ANY)
        vmem = pl.BlockSpec(memory_space=pltpu.VMEM)
        dma = pltpu.SemaphoreType.DMA
        return pl.pallas_call(
            functools.partial(kernel, dims, runs),
            out_shape=pltpu.VMEM((months, month_total), jnp.float32),
            in_specs=[hbm, hbm, hbm, hbm],
            out_specs=vmem,
            scratch_shapes=[
                pltpu.VMEM((rows * months, lon_count), jnp.bfloat16),
                pltpu.VMEM(table.shape, jnp.bfloat16),
                pltpu.VMEM(starts.shape[1:], jnp.float32),
                pltpu.VMEM(lats.shape, jnp.float32),
                pltpu.VMEM((device_total * longest * high, LANES), jnp.float32),
                pltpu.VMEM((device_total, slots * bands, high // bands, LANES), jnp.bfloat16),
                pltpu.VMEM((device_total, slots * bands, high // bands, LANES), jnp.bfloat16),
                pltpu.VMEM((lat_total // LANES, slot_rows * depth, LANES), jnp.float32),
                pltpu.VMEM((width, width), jnp.float32),
                pltpu.VMEM((pieces, PIECE, month_total), jnp.float32),
                pltpu.VMEM((device_total, PIECE, month_total), jnp.float32),
                pltpu.VMEM((PIECE, month_total), jnp.float32),
                pltpu.VMEM((pieces, PIECE, month_total), jnp.float32),
                dma,
                dma((len(phases),)),
                dma((2,)),
                dma((len(phases),)),
                dma((len(phases),)),
                dma((4,)),
            ],
            compiler_params=pltpu.CompilerParams(
                collective_id=0, has_side_effects=True, vmem_limit_bytes=60 * 1024 * 1024
            ),
        )(fields.reshape(rows * months, lon_count), table, starts, lats)

    return jax.shard_map(
        local, mesh=mesh, in_specs=(P("lat", "tm", None),), out_specs=P("tm", None), check_vma=False
    )
```

```python
import functools
import math

import jax
import jax.numpy as jnp
import numpy as np
from jax import lax
from jax.experimental import pallas as pl
from jax.experimental.pallas import tpu as pltpu
from jax.sharding import PartitionSpec as P

TRUNC = 341
LANES = 128
HALF = 64
PIECE = 8
PHASES = 3
MESH = pl.DeviceIdType.MESH


def phase_bounds(slots):
    length = -(-slots // PHASES)
    return [(low, min(low + length, slots)) for low in range(0, slots, length)]


def rank_of(lat, tm, lat_devices, tm_devices):
    hemisphere = lat_devices // 2
    return ((lat % hemisphere) * tm_devices + tm) * 2 + lat // hemisphere


def ranks(lat_devices, tm_devices):
    device = np.arange(lat_devices * tm_devices)
    return rank_of(device // tm_devices, device % tm_devices, lat_devices, tm_devices)


def twiddle_table(rank, slots, lon_count):
    device_total = len(rank)
    longitude = np.arange(lon_count)
    parts = []
    for low, top in phase_bounds(slots):
        wave = (np.arange(low, top)[None, :] * device_total + rank[:, None]).reshape(-1, 1)
        phase = 2.0 * math.pi * ((wave * longitude) % lon_count) / lon_count
        active = (wave <= TRUNC) / math.sqrt(lon_count)
        parts += [np.cos(phase) * active, -np.sin(phase) * active]
    return np.concatenate(parts).astype(np.float32).astype(jnp.bfloat16)


def start_table(rank, slots, slot_rows):
    device_total = len(rank)
    table = np.zeros((device_total, slot_rows), np.float64)
    for device in range(device_total):
        for slot in range(slot_rows):
            order = min(slot, slots - 1) * device_total + int(rank[device])
            table[device, slot] = 0.5 * (
                math.log(0.5)
                + math.lgamma(order + 1.5)
                - math.lgamma(1.5)
                - math.lgamma(order + 1.0)
            )
    table = np.broadcast_to(table[:, :, None], (device_total, slot_rows, LANES))
    return table.astype(np.float32)


def needed_slots(lat_devices, device_total, slots, rows, bands):
    counts = []
    order = np.arange(slots * device_total)
    rise = np.array(
        [math.lgamma(m + 1.5) - math.lgamma(1.5) - math.lgamma(m + 1.0) for m in order]
    )
    for device in range(lat_devices):
        lat = device * rows + np.arange(rows)
        sine = np.sin(math.pi * (lat + 0.5) / (lat_devices * rows))
        start = 0.5 * (math.log(0.5) + rise[:, None]) + order[:, None] * np.log(sine)[None, :]
        used = (start > -70.5) & (order <= TRUNC)[:, None]
        used = used.reshape(slots, device_total, bands, -1).any(axis=(1, 3))
        counts.append(
            tuple(
                int(np.max(np.nonzero(used[:, band])[0])) + 1 if used[:, band].any() else 0
                for band in range(bands)
            )
        )
    runs = []
    for device, count in enumerate(counts):
        if runs and runs[-1][2] == count:
            runs[-1][1] = device + 1
        else:
            runs.append([device, device + 1, count])
    return tuple(tuple(run) for run in runs)


def lat_table(lat_total, share):
    lat = np.arange(lat_total).reshape(lat_total // share, share).T.reshape(-1)
    theta = math.pi * (lat + 0.5) / lat_total
    table = np.stack([np.cos(theta), np.log(np.sin(theta)), math.pi * np.sin(theta) / lat_total])
    return table.reshape(3, lat_total // LANES, LANES).astype(np.float32)


def kernel(
    dims,
    runs,
    x_hbm,
    table_hbm,
    start_hbm,
    lat_hbm,
    out_ref,
    x_ref,
    table_ref,
    start_ref,
    lat_ref,
    spread,
    outbox,
    inbox,
    legendre,
    gram_ref,
    local_gram,
    parts,
    own_sum,
    full,
    x_sem,
    table_sem,
    small_sem,
    send_sem,
    recv_sem,
    tail_sem,
):
    lat_devices, tm_devices, rows, months, lon_count, slots, slot_rows, depth = dims
    device_total = lat_devices * tm_devices
    share = HALF // months
    high = rows // share
    lat_total = lat_devices * rows
    lat_groups = lat_total // LANES
    month_total = months * tm_devices
    group = months // PIECE
    pieces = group * tm_devices
    lat_me = lax.axis_index("lat")
    tm_me = lax.axis_index("tm")
    me = lat_me * tm_devices + tm_me
    rank_me = rank_of(lat_me, tm_me, lat_devices, tm_devices)

    phases = phase_bounds(slots)

    def each_peer(act):
        def row(lat):
            for tm in range(tm_devices):
                act(lat, tm)

        pl.loop(lat_me + 1, lat_devices)(row)
        pl.loop(0, lat_me)(row)
        for tm in range(tm_devices):

            @pl.when(tm_me != tm)
            def _():
                act(lat_me, tm)

    barrier = pltpu.get_barrier_semaphore()
    each_peer(
        lambda lat, tm: pl.semaphore_signal(
            barrier, inc=1, device_id=(lat, tm), device_id_type=MESH
        )
    )

    x_copy = pltpu.make_async_copy(x_hbm, x_ref, x_sem)
    x_copy.start()

    def table_copy(phase):
        low, top = phases[phase]
        span = pl.ds(2 * device_total * low, 2 * device_total * (top - low))
        return pltpu.make_async_copy(table_hbm.at[span], table_ref.at[span], table_sem.at[phase])

    for phase in range(len(phases)):
        table_copy(phase).start()

    start_copy = pltpu.make_async_copy(start_hbm.at[me], start_ref, small_sem.at[0])
    start_copy.start()
    lat_copy = pltpu.make_async_copy(lat_hbm, lat_ref, small_sem.at[1])
    lat_copy.start()

    bands = len(runs[0][2])
    band_rows = high // bands
    for first, last, counts in runs:
        for band, count in enumerate(counts):
            if count < slots:

                @pl.loop(first * tm_devices, last * tm_devices)
                def _(source):
                    for slot in range(count, slots):
                        inbox[source, slot * bands + band] = jnp.zeros(
                            (band_rows, LANES), jnp.bfloat16
                        )

    last_order = (slots - 1) * device_total
    last_holders = min(TRUNC + 1 - last_order, device_total)

    def holds_last(lat, tm):
        return last_order + rank_of(lat, tm, lat_devices, tm_devices) <= TRUNC

    def splits(phase):
        return phases[phase][1] == slots and last_holders < device_total

    if last_holders < device_total:

        @pl.when(jnp.logical_not(holds_last(lat_me, tm_me)))
        def _():
            inbox[:, (slots - 1) * bands :] = jnp.zeros(
                (device_total, bands, band_rows, LANES), jnp.bfloat16
            )

    def pieces_of(phase, counts, held):
        low, top = phases[phase]
        if not held:
            top = min(top, slots - 1)
        found = []
        shared = min(min(counts), top)
        if shared > low:
            found.append((low * bands, (shared - low) * bands))
        for band, count in enumerate(counts):
            for slot in range(max(low, min(counts)), min(count, top)):
                found.append((slot * bands + band, 1))
        return found

    def blocks_of(phase, counts, held):
        return sum(length for first, length in pieces_of(phase, counts, held))

    def leaving(phase, counts, held):
        kept = blocks_of(phase, counts, True) * last_holders
        rest = blocks_of(phase, counts, False) * (device_total - last_holders)
        return kept + rest - blocks_of(phase, counts, held)

    def arriving(phase, counts, held):
        total = sum(
            (last - first) * tm_devices * blocks_of(phase, counts, held)
            for first, last, counts in runs
        )
        return total - blocks_of(phase, counts, held)

    def each_case(phase, held, act):
        if splits(phase):
            pl.when(held)(lambda: act(True))
            pl.when(jnp.logical_not(held))(lambda: act(False))
        else:
            act(True)

    def wait_blocks(semaphore, count):
        if count:
            span = spread.at[pl.ds(0, count * band_rows // 2)]
            pltpu.make_async_copy(span, span, semaphore).wait()

    def each_class(act):
        for first, last, counts in runs:

            @pl.when((lat_me >= first) & (lat_me < last))
            def _():
                act(counts)

    def transform(phase):
        low, top = phases[phase]
        group_rows = device_total * (top - low)
        lower = lax.broadcasted_iota(jnp.int32, (group_rows, LANES), 1) < HALF
        table_copy(phase).wait()
        values = lax.dot_general(
            table_ref[2 * device_total * low : 2 * device_total * top],
            x_ref[...],
            (((1,), (1,)), ((), ())),
            preferred_element_type=jnp.float32,
        )
        for block in range(rows * months // LANES):
            cosine = values[:group_rows, block * LANES : (block + 1) * LANES]
            sine = values[group_rows:, block * LANES : (block + 1) * LANES]
            even = jnp.where(lower, cosine, pltpu.roll(sine, HALF, 1))
            odd = jnp.where(lower, pltpu.roll(cosine, HALF, 1), sine)
            spread[pl.ds(2 * block, group_rows, stride=high), :] = even
            spread[pl.ds(2 * block + 1, group_rows, stride=high), :] = odd
        packed = spread[: group_rows * high].astype(jnp.bfloat16)
        outbox[:, low * bands : top * bands] = packed.reshape(
            device_total, (top - low) * bands, band_rows, LANES
        )

    def exchange(phase, piece, lat, tm):
        span = pl.ds(*piece)
        return pltpu.make_async_remote_copy(
            src_ref=outbox.at[lat * tm_devices + tm, span],
            dst_ref=inbox.at[me, span],
            send_sem=send_sem.at[phase],
            recv_sem=recv_sem.at[phase],
            device_id=(lat, tm),
            device_id_type=MESH,
        )

    def send(phase):
        def send_class(counts):
            def send_to(lat, tm):
                def go(held):
                    for piece in pieces_of(phase, counts, held):
                        exchange(phase, piece, lat, tm).start()

                each_case(phase, holds_last(lat, tm), go)

            if pieces_of(phase, counts, True):
                each_peer(send_to)

        each_class(send_class)

    held_here = holds_last(lat_me, tm_me)

    def wait_moved(phase, semaphore, amount):
        each_class(
            lambda counts: each_case(
                phase,
                held_here,
                lambda held: wait_blocks(semaphore.at[phase], amount(phase, counts, held)),
            )
        )

    with jax.named_scope("xwait"):
        x_copy.wait()
    for phase in range(len(phases)):
        with jax.named_scope(f"transform{phase}"):
            transform(phase)
        if phase == 0:
            with jax.named_scope("barrier"):
                pl.semaphore_wait(barrier, device_total - 1)
        with jax.named_scope(f"send{phase}"):
            send(phase)

    inbox[me] = outbox[me]

    start_copy.wait()
    lat_copy.wait()

    halves = slot_rows // 8
    sub = lax.broadcasted_iota(jnp.int32, (8, LANES), 0)
    slot_of = [sub + 8 * half for half in range(halves)]
    order_int = [slot * device_total + rank_me for slot in slot_of]
    order = [value.astype(jnp.float32) for value in order_int]
    cosine_lat = [jnp.broadcast_to(lat_ref[0, pl.ds(g, 1), :], (8, LANES)) for g in range(lat_groups)]
    current = []
    scale = []
    for half in range(halves):
        factor = jnp.where(order_int[half] > 0, math.sqrt(2.0), 1.0)
        for g in range(lat_groups):
            log_start = (
                start_ref[pl.ds(8 * half, 8), :]
                + order[half] * jnp.broadcast_to(lat_ref[1, pl.ds(g, 1), :], (8, LANES))
            )
            taper = jnp.clip((log_start + 70.0) / 10.0, 0.0, 1.0)
            current.append(jnp.exp(jnp.maximum(log_start, -80.0)) * taper)
            scale.append(factor * jnp.broadcast_to(lat_ref[2, pl.ds(g, 1), :], (8, LANES)))

    def store(offset, values):
        for half in range(halves):
            keep = (order_int[half] + offset <= TRUNC) & (slot_of[half] < slots)
            for g in range(lat_groups):
                index = half * lat_groups + g
                value = jnp.where(keep, values[index] * scale[index], 0.0)
                legendre[g, pl.ds(8 * half * depth + offset, 8, stride=depth), :] = value

    store(0, current)

    def advance(offset, carry):
        now, before, backs = carry
        real = lax.convert_element_type(offset, jnp.float32)
        following = []
        next_backs = []
        for half in range(halves):
            degree = order[half] + real
            ratio = (4.0 * degree * degree - 1.0) / (real * (order[half] + degree))
            top = jnp.sqrt(ratio)
            next_backs.append(1.0 / top)
            for g in range(lat_groups):
                index = half * lat_groups + g
                following.append(
                    top * (cosine_lat[g] * now[index] - backs[half] * before[index])
                )
        store(offset, following)
        return following, now, next_backs

    zero = jnp.zeros((8, LANES), jnp.float32)
    with jax.named_scope("legendre"):
        lax.fori_loop(
            1,
            depth,
            advance,
            (current, [zero] * len(current), [zero] * halves),
            unroll=7,
        )

    per_share = lat_groups // share
    width = tm_devices * LANES

    def coefficients(slot, height):
        received = jnp.concatenate(
            [
                jnp.concatenate(
                    [
                        inbox[lat_device * tm_devices + tm, slot * bands : (slot + 1) * bands].reshape(
                            high, LANES
                        )
                        for lat_device in range(lat_devices)
                    ],
                    axis=0,
                )
                for tm in range(tm_devices)
            ],
            axis=1,
        )
        share_of = lax.broadcasted_iota(jnp.int32, (height, width), 1) % HALF // months
        first = slot * depth
        merged = None
        for part in range(share):
            basis = jnp.concatenate(
                [
                    legendre[part * per_share + g, first : first + height, :].astype(jnp.bfloat16)
                    for g in range(per_share)
                ],
                axis=1,
            )
            product = jnp.dot(basis, received, preferred_element_type=jnp.float32)
            merged = product if part == 0 else jnp.where(share_of == part, product, merged)
        total = merged
        for part in range(1, share):
            total = total + pltpu.roll(merged, width - part * months, 1)
        return jnp.where(share_of == 0, total, 0.0).astype(jnp.bfloat16)

    for phase, (low, top) in enumerate(phases):
        with jax.named_scope(f"recv{phase}"):
            wait_moved(phase, recv_sem, arriving)
        with jax.named_scope(f"slots{phase}"):
            heights = [
                min(-(-(TRUNC + 1 - slot * device_total) // 16) * 16, depth)
                for slot in range(low, top)
            ]
            values = jnp.concatenate(
                [coefficients(low + index, height) for index, height in enumerate(heights)],
                axis=0,
            )
            product = lax.dot_general(
                values, values, (((0,), (0,)), ((), ())), preferred_element_type=jnp.float32
            )
            gram_ref[...] = product if phase == 0 else gram_ref[...] + product

    gram = None
    for part in range(2):
        across = jnp.concatenate(
            [
                gram_ref[pl.ds(tm * LANES + part * HALF, months), :]
                for tm in range(tm_devices)
            ],
            axis=0,
        )
        block = jnp.concatenate(
            [
                across[:, tm * LANES + part * HALF : tm * LANES + part * HALF + months]
                for tm in range(tm_devices)
            ],
            axis=1,
        )
        gram = block if gram is None else gram + block
    on_diagonal = lax.broadcasted_iota(jnp.int32, gram.shape, 0) == lax.broadcasted_iota(
        jnp.int32, gram.shape, 1
    )
    diagonal = jnp.sum(jnp.where(on_diagonal, gram, 0.0), axis=0, keepdims=True)
    local_gram[:, :PIECE] = gram.reshape(pieces, PIECE, month_total)
    local_gram[:, PIECE:] = jnp.broadcast_to(diagonal[None], (pieces, 1, month_total))

    first_lat = lat_me // group * group
    place = lat_me % group
    local_me = place * tm_devices + tm_me

    def send_part(other, tm):
        return pltpu.make_async_remote_copy(
            src_ref=local_gram.at[tm * group + other],
            dst_ref=parts.at[local_me],
            send_sem=tail_sem.at[0],
            recv_sem=tail_sem.at[1],
            device_id=(first_lat + other, tm),
            device_id_type=MESH,
        )

    def send_sum(lat):
        return pltpu.make_async_remote_copy(
            src_ref=own_sum,
            dst_ref=full.at[lat_me],
            send_sem=tail_sem.at[2],
            recv_sem=tail_sem.at[3],
            device_id=(lat, tm_me),
            device_id_type=MESH,
        )

    def wait_tail(index, ref, count):
        if count:
            span = ref.at[pl.ds(0, count)]
            pltpu.make_async_copy(span, span, tail_sem.at[index]).wait()

    for other in range(group):
        for tm in range(tm_devices):

            @pl.when((other != place) | (tm != tm_me))
            def _():
                send_part(other, tm).start()

    with jax.named_scope("waitsend"):
        for phase in range(len(phases)):
            wait_moved(phase, send_sem, leaving)

    parts[local_me] = local_gram[tm_me * group + place]
    with jax.named_scope("owner"):
        wait_tail(1, parts, pieces - 1)
    total = jnp.sum(parts[...], axis=0)
    own_sum[...] = total
    full[lat_me] = total

    @pl.loop(1, lat_devices)
    def _(step):
        send_sum(lax.rem(lat_me + step, lat_devices)).start()

    with jax.named_scope("waitsum"):
        wait_tail(3, full, lat_devices - 1)

    with jax.named_scope("norm"):
        sums = full[:group]
        for block in range(group, lat_devices, group):
            sums = sums + full[block : block + group]
        trace = jnp.sum(sums[0, PIECE:])
        here = sums[:, :PIECE].reshape(months, month_total)
        out_ref[...] = month_total * here / (trace + 1e-06)

    with jax.named_scope("drain"):
        wait_tail(0, local_gram, pieces - 1)
        wait_tail(2, full, lat_devices - 1)


def solution(mesh):
    lat_devices = mesh.shape["lat"]
    tm_devices = mesh.shape["tm"]
    device_total = lat_devices * tm_devices
    slots = -(-(TRUNC + 1) // device_total)
    slot_rows = -(-slots // 8) * 8
    depth = -(-(TRUNC + 1) // 8) * 8

    def local(fields):
        rows, months, lon_count = fields.shape
        month_total = months * tm_devices
        lat_total = rows * lat_devices
        share = HALF // months
        high = rows // share
        pieces = month_total // PIECE
        width = tm_devices * LANES
        dims = (lat_devices, tm_devices, rows, months, lon_count, slots, slot_rows, depth)
        rank = ranks(lat_devices, tm_devices)
        table = jnp.asarray(twiddle_table(rank, slots, lon_count))
        starts = jnp.asarray(start_table(rank, slots, slot_rows))
        lats = jnp.asarray(lat_table(lat_total, share))
        bands = 2 if high % 16 == 0 else 1
        runs = needed_slots(lat_devices, device_total, slots, rows, bands)
        phases = phase_bounds(slots)
        longest = max(top - low for low, top in phases)
        hbm = pl.BlockSpec(memory_space=pl.ANY)
        vmem = pl.BlockSpec(memory_space=pltpu.VMEM)
        dma = pltpu.SemaphoreType.DMA
        return pl.pallas_call(
            functools.partial(kernel, dims, runs),
            out_shape=pltpu.VMEM((months, month_total), jnp.float32),
            in_specs=[hbm, hbm, hbm, hbm],
            out_specs=vmem,
            scratch_shapes=[
                pltpu.VMEM((rows * months, lon_count), jnp.bfloat16),
                pltpu.VMEM(table.shape, jnp.bfloat16),
                pltpu.VMEM(starts.shape[1:], jnp.float32),
                pltpu.VMEM(lats.shape, jnp.float32),
                pltpu.VMEM((device_total * longest * high, LANES), jnp.float32),
                pltpu.VMEM((device_total, slots * bands, high // bands, LANES), jnp.bfloat16),
                pltpu.VMEM((device_total, slots * bands, high // bands, LANES), jnp.bfloat16),
                pltpu.VMEM((lat_total // LANES, slot_rows * depth, LANES), jnp.float32),
                pltpu.VMEM((width, width), jnp.float32),
                pltpu.VMEM((pieces, PIECE + 1, month_total), jnp.float32),
                pltpu.VMEM((pieces, PIECE + 1, month_total), jnp.float32),
                pltpu.VMEM((PIECE + 1, month_total), jnp.float32),
                pltpu.VMEM((lat_devices, PIECE + 1, month_total), jnp.float32),
                dma,
                dma((len(phases),)),
                dma((2,)),
                dma((len(phases),)),
                dma((len(phases),)),
                dma((4,)),
            ],
            compiler_params=pltpu.CompilerParams(
                collective_id=0, has_side_effects=True, vmem_limit_bytes=60 * 1024 * 1024
            ),
        )(fields.reshape(rows * months, lon_count), table, starts, lats)

    return jax.shard_map(
        local, mesh=mesh, in_specs=(P("lat", "tm", None),), out_specs=P("tm", None), check_vma=False
    )
```

```python
import functools
import math

import jax
import jax.numpy as jnp
import numpy as np
from jax import lax
from jax.experimental import pallas as pl
from jax.experimental.pallas import tpu as pltpu
from jax.sharding import PartitionSpec as P

TRUNC = 341
LANES = 128
HALF = 64
PIECE = 8
PHASES = 3
MESH = pl.DeviceIdType.MESH


def phase_bounds(slots):
    length = -(-slots // PHASES)
    return [(low, min(low + length, slots)) for low in range(0, slots, length)]


def rank_of(lat, tm, lat_devices, tm_devices):
    hemisphere = lat_devices // 2
    return ((lat % hemisphere) * tm_devices + tm) * 2 + lat // hemisphere


def ranks(lat_devices, tm_devices):
    device = np.arange(lat_devices * tm_devices)
    return rank_of(device // tm_devices, device % tm_devices, lat_devices, tm_devices)


def twiddle_table(rank, slots, lon_count):
    device_total = len(rank)
    longitude = np.arange(lon_count)
    parts = []
    for low, top in phase_bounds(slots):
        wave = (np.arange(low, top)[None, :] * device_total + rank[:, None]).reshape(-1, 1)
        phase = 2.0 * math.pi * ((wave * longitude) % lon_count) / lon_count
        active = (wave <= TRUNC) / math.sqrt(lon_count)
        parts += [np.cos(phase) * active, -np.sin(phase) * active]
    return np.concatenate(parts).astype(np.float32).astype(jnp.bfloat16)


def start_table(rank, slots, slot_rows):
    device_total = len(rank)
    table = np.zeros((device_total, slot_rows), np.float64)
    for device in range(device_total):
        for slot in range(slot_rows):
            order = min(slot, slots - 1) * device_total + int(rank[device])
            table[device, slot] = 0.5 * (
                math.log(0.5)
                + math.lgamma(order + 1.5)
                - math.lgamma(1.5)
                - math.lgamma(order + 1.0)
            )
    table = np.broadcast_to(table[:, :, None], (device_total, slot_rows, LANES))
    return table.astype(np.float32)


def needed_slots(lat_devices, device_total, slots, rows, bands):
    counts = []
    order = np.arange(slots * device_total)
    rise = np.array(
        [math.lgamma(m + 1.5) - math.lgamma(1.5) - math.lgamma(m + 1.0) for m in order]
    )
    for device in range(lat_devices):
        lat = device * rows + np.arange(rows)
        sine = np.sin(math.pi * (lat + 0.5) / (lat_devices * rows))
        start = 0.5 * (math.log(0.5) + rise[:, None]) + order[:, None] * np.log(sine)[None, :]
        used = (start > -70.5) & (order <= TRUNC)[:, None]
        used = used.reshape(slots, device_total, bands, -1).any(axis=(1, 3))
        counts.append(
            tuple(
                int(np.max(np.nonzero(used[:, band])[0])) + 1 if used[:, band].any() else 0
                for band in range(bands)
            )
        )
    runs = []
    for device, count in enumerate(counts):
        if runs and runs[-1][2] == count:
            runs[-1][1] = device + 1
        else:
            runs.append([device, device + 1, count])
    return tuple(tuple(run) for run in runs)


def relay_routes(lat_devices, group, runs, first_top):
    if lat_devices != 4 * group or group % 2:
        return ()
    routes = []
    for source, via in ((group // 2, 0), (lat_devices - 1 - group // 2, lat_devices - 1)):
        for first, last, counts in runs:
            if (first, last) == (source, source + 1) and 0 < max(counts) <= first_top:
                routes.append((source, via, counts))
    return tuple(routes)


def lat_table(lat_total, share):
    lat = np.arange(lat_total).reshape(lat_total // share, share).T.reshape(-1)
    theta = math.pi * (lat + 0.5) / lat_total
    table = np.stack([np.cos(theta), np.log(np.sin(theta)), math.pi * np.sin(theta) / lat_total])
    return table.reshape(3, lat_total // LANES, LANES).astype(np.float32)


def kernel(
    dims,
    runs,
    routes,
    x_hbm,
    table_hbm,
    start_hbm,
    lat_hbm,
    out_ref,
    x_ref,
    table_ref,
    start_ref,
    lat_ref,
    spread,
    outbox,
    inbox,
    relay,
    legendre,
    gram_ref,
    local_gram,
    parts,
    own_sum,
    full,
    x_sem,
    table_sem,
    small_sem,
    send_sem,
    recv_sem,
    relay_sem,
    tail_sem,
):
    lat_devices, tm_devices, rows, months, lon_count, slots, slot_rows, depth = dims
    device_total = lat_devices * tm_devices
    share = HALF // months
    high = rows // share
    lat_total = lat_devices * rows
    lat_groups = lat_total // LANES
    month_total = months * tm_devices
    group = months // PIECE
    pieces = group * tm_devices
    lat_me = lax.axis_index("lat")
    tm_me = lax.axis_index("tm")
    me = lat_me * tm_devices + tm_me
    rank_me = rank_of(lat_me, tm_me, lat_devices, tm_devices)

    phases = phase_bounds(slots)

    def each_peer(act):
        def row(lat):
            for tm in range(tm_devices):
                act(lat, tm)

        pl.loop(lat_me + 1, lat_devices)(row)
        pl.loop(0, lat_me)(row)
        for tm in range(tm_devices):

            @pl.when(tm_me != tm)
            def _():
                act(lat_me, tm)

    barrier = pltpu.get_barrier_semaphore()
    each_peer(
        lambda lat, tm: pl.semaphore_signal(
            barrier, inc=1, device_id=(lat, tm), device_id_type=MESH
        )
    )

    hemisphere = lat_devices // 2

    def each_target(act):
        @pl.loop(0, lat_devices)
        def _(step):
            if lat_devices & (lat_devices - 1):
                lat = lax.rem(lat_me + step, lat_devices)
            else:
                lat = lat_me ^ ((step // 2) ^ ((step + 1) % 2 * hemisphere))
            for tm in range(tm_devices):

                @pl.when((lat != lat_me) | (tm != tm_me))
                def _():
                    act(lat, tm)

    x_copy = pltpu.make_async_copy(x_hbm, x_ref, x_sem)
    x_copy.start()

    def table_copy(phase):
        low, top = phases[phase]
        span = pl.ds(2 * device_total * low, 2 * device_total * (top - low))
        return pltpu.make_async_copy(table_hbm.at[span], table_ref.at[span], table_sem.at[phase])

    for phase in range(len(phases)):
        table_copy(phase).start()

    start_copy = pltpu.make_async_copy(start_hbm.at[me], start_ref, small_sem.at[0])
    start_copy.start()
    lat_copy = pltpu.make_async_copy(lat_hbm, lat_ref, small_sem.at[1])
    lat_copy.start()

    bands = len(runs[0][2])
    band_rows = high // bands
    for first, last, counts in runs:
        for band, count in enumerate(counts):
            if count < slots:

                @pl.loop(first * tm_devices, last * tm_devices)
                def _(source):
                    for slot in range(count, slots):
                        inbox[source, slot * bands + band] = jnp.zeros(
                            (band_rows, LANES), jnp.bfloat16
                        )

    last_order = (slots - 1) * device_total
    last_holders = min(TRUNC + 1 - last_order, device_total)

    def holds_last(lat, tm):
        return last_order + rank_of(lat, tm, lat_devices, tm_devices) <= TRUNC

    def splits(phase):
        return phases[phase][1] == slots and last_holders < device_total

    if last_holders < device_total:

        @pl.when(jnp.logical_not(holds_last(lat_me, tm_me)))
        def _():
            inbox[:, (slots - 1) * bands :] = jnp.zeros(
                (device_total, bands, band_rows, LANES), jnp.bfloat16
            )

    def pieces_of(phase, counts, held):
        low, top = phases[phase]
        if not held:
            top = min(top, slots - 1)
        found = []
        shared = min(min(counts), top)
        if shared > low:
            found.append((low * bands, (shared - low) * bands))
        for band, count in enumerate(counts):
            for slot in range(max(low, min(counts)), min(count, top)):
                found.append((slot * bands + band, 1))
        return found

    def blocks_of(phase, counts, held):
        return sum(length for first, length in pieces_of(phase, counts, held))

    sources = [source for source, via, counts in routes]

    def relays(phase, first):
        return phase == 0 and first in sources

    def leaving(phase, first, counts, held):
        if relays(phase, first):
            return blocks_of(phase, counts, held) * (device_total // 2 - 1)
        kept = blocks_of(phase, counts, True) * last_holders
        rest = blocks_of(phase, counts, False) * (device_total - last_holders)
        return kept + rest - blocks_of(phase, counts, held)

    def arriving(phase, first, counts, held):
        total = sum(
            (last - first) * tm_devices * blocks_of(phase, counts, held)
            for first, last, counts in runs
        )
        return total - blocks_of(phase, counts, held)

    def each_case(phase, held, act):
        if splits(phase):
            pl.when(held)(lambda: act(True))
            pl.when(jnp.logical_not(held))(lambda: act(False))
        else:
            act(True)

    def wait_blocks(semaphore, count):
        if count:
            span = spread.at[pl.ds(0, count * band_rows // 2)]
            pltpu.make_async_copy(span, span, semaphore).wait()

    def each_class(act):
        for first, last, counts in runs:

            @pl.when((lat_me >= first) & (lat_me < last))
            def _():
                act(first, counts)

    def transform(phase):
        low, top = phases[phase]
        group_rows = device_total * (top - low)
        lower = lax.broadcasted_iota(jnp.int32, (group_rows, LANES), 1) < HALF
        table_copy(phase).wait()
        values = lax.dot_general(
            table_ref[2 * device_total * low : 2 * device_total * top],
            x_ref[...],
            (((1,), (1,)), ((), ())),
            preferred_element_type=jnp.float32,
        )
        for block in range(rows * months // LANES):
            cosine = values[:group_rows, block * LANES : (block + 1) * LANES]
            sine = values[group_rows:, block * LANES : (block + 1) * LANES]
            even = jnp.where(lower, cosine, pltpu.roll(sine, HALF, 1))
            odd = jnp.where(lower, pltpu.roll(cosine, HALF, 1), sine)
            spread[pl.ds(2 * block, group_rows, stride=high), :] = even
            spread[pl.ds(2 * block + 1, group_rows, stride=high), :] = odd
        packed = spread[: group_rows * high].astype(jnp.bfloat16)
        outbox[:, low * bands : top * bands] = packed.reshape(
            device_total, (top - low) * bands, band_rows, LANES
        )

    def exchange(phase, piece, lat, tm):
        span = pl.ds(*piece)
        return pltpu.make_async_remote_copy(
            src_ref=outbox.at[lat * tm_devices + tm, span],
            dst_ref=inbox.at[me, span],
            send_sem=send_sem.at[phase],
            recv_sem=recv_sem.at[phase],
            device_id=(lat, tm),
            device_id_type=MESH,
        )

    def across(source):
        return hemisphere - source // hemisphere * hemisphere

    def to_relay(source, via):
        span = pl.ds(across(source) * tm_devices, hemisphere * tm_devices)
        return pltpu.make_async_remote_copy(
            src_ref=outbox.at[span, pl.ds(0, relay.shape[1])],
            dst_ref=relay,
            send_sem=relay_sem.at[0],
            recv_sem=relay_sem.at[1],
            device_id=(via, tm_me),
            device_id_type=MESH,
        )

    def from_relay(source, counts):
        @pl.loop(0, hemisphere * tm_devices)
        def _(index):
            for piece in pieces_of(0, counts, True):
                span = pl.ds(*piece)
                pltpu.make_async_remote_copy(
                    src_ref=relay.at[index, span],
                    dst_ref=inbox.at[source * tm_devices + tm_me, span],
                    send_sem=relay_sem.at[2],
                    recv_sem=recv_sem.at[0],
                    device_id=(across(source) + index // tm_devices, index % tm_devices),
                    device_id_type=MESH,
                ).start()

    def send(phase):
        def send_class(start, counts):
            def send_to(lat, tm):
                def go(held):
                    for piece in pieces_of(phase, counts, held):
                        exchange(phase, piece, lat, tm).start()

                each_case(phase, holds_last(lat, tm), go)

            def send_near(lat, tm):
                pl.when(lat // hemisphere == start // hemisphere)(lambda: send_to(lat, tm))

            if relays(phase, start):
                for source, via, _ in routes:
                    if source == start:
                        to_relay(source, via).start()
                each_target(send_near)
            elif pieces_of(phase, counts, True):
                each_target(send_to)

        each_class(send_class)

    held_here = holds_last(lat_me, tm_me)

    def wait_moved(phase, semaphore, amount):
        each_class(
            lambda first, counts: each_case(
                phase,
                held_here,
                lambda held: wait_blocks(semaphore.at[phase], amount(phase, first, counts, held)),
            )
        )

    with jax.named_scope("xwait"):
        x_copy.wait()
    for phase in range(len(phases)):
        with jax.named_scope(f"transform{phase}"):
            transform(phase)
        if phase == 0:
            with jax.named_scope("barrier"):
                pl.semaphore_wait(barrier, device_total - 1)
        with jax.named_scope(f"send{phase}"):
            send(phase)

    inbox[me] = outbox[me]

    start_copy.wait()
    lat_copy.wait()

    halves = slot_rows // 8
    sub = lax.broadcasted_iota(jnp.int32, (8, LANES), 0)
    slot_of = [sub + 8 * half for half in range(halves)]
    order_int = [slot * device_total + rank_me for slot in slot_of]
    order = [value.astype(jnp.float32) for value in order_int]
    cosine_lat = [jnp.broadcast_to(lat_ref[0, pl.ds(g, 1), :], (8, LANES)) for g in range(lat_groups)]
    current = []
    scale = []
    for half in range(halves):
        factor = jnp.where(order_int[half] > 0, math.sqrt(2.0), 1.0)
        for g in range(lat_groups):
            log_start = (
                start_ref[pl.ds(8 * half, 8), :]
                + order[half] * jnp.broadcast_to(lat_ref[1, pl.ds(g, 1), :], (8, LANES))
            )
            taper = jnp.clip((log_start + 70.0) / 10.0, 0.0, 1.0)
            current.append(jnp.exp(jnp.maximum(log_start, -80.0)) * taper)
            scale.append(factor * jnp.broadcast_to(lat_ref[2, pl.ds(g, 1), :], (8, LANES)))

    def store(offset, values):
        for half in range(halves):
            keep = (order_int[half] + offset <= TRUNC) & (slot_of[half] < slots)
            for g in range(lat_groups):
                index = half * lat_groups + g
                value = jnp.where(keep, values[index] * scale[index], 0.0)
                legendre[g, pl.ds(8 * half * depth + offset, 8, stride=depth), :] = value

    store(0, current)

    def advance(offset, carry):
        now, before, backs = carry
        real = lax.convert_element_type(offset, jnp.float32)
        following = []
        next_backs = []
        for half in range(halves):
            degree = order[half] + real
            ratio = (4.0 * degree * degree - 1.0) / (real * (order[half] + degree))
            top = jnp.sqrt(ratio)
            next_backs.append(1.0 / top)
            for g in range(lat_groups):
                index = half * lat_groups + g
                following.append(
                    top * (cosine_lat[g] * now[index] - backs[half] * before[index])
                )
        store(offset, following)
        return following, now, next_backs

    zero = jnp.zeros((8, LANES), jnp.float32)
    with jax.named_scope("legendre"):
        lax.fori_loop(
            1,
            depth,
            advance,
            (current, [zero] * len(current), [zero] * halves),
            unroll=7,
        )

    def wait_relay(index, ref):
        pltpu.make_async_copy(ref, ref, relay_sem.at[index]).wait()

    with jax.named_scope("relay"):
        for source, via, counts in routes:

            @pl.when(lat_me == via)
            def _():
                wait_relay(1, relay)
                from_relay(source, counts)

    per_share = lat_groups // share
    width = tm_devices * LANES

    def coefficients(slot, height):
        received = jnp.concatenate(
            [
                jnp.concatenate(
                    [
                        inbox[lat_device * tm_devices + tm, slot * bands : (slot + 1) * bands].reshape(
                            high, LANES
                        )
                        for lat_device in range(lat_devices)
                    ],
                    axis=0,
                )
                for tm in range(tm_devices)
            ],
            axis=1,
        )
        share_of = lax.broadcasted_iota(jnp.int32, (height, width), 1) % HALF // months
        first = slot * depth
        merged = None
        for part in range(share):
            basis = jnp.concatenate(
                [
                    legendre[part * per_share + g, first : first + height, :].astype(jnp.bfloat16)
                    for g in range(per_share)
                ],
                axis=1,
            )
            product = jnp.dot(basis, received, preferred_element_type=jnp.float32)
            merged = product if part == 0 else jnp.where(share_of == part, product, merged)
        total = merged
        for part in range(1, share):
            total = total + pltpu.roll(merged, width - part * months, 1)
        return jnp.where(share_of == 0, total, 0.0).astype(jnp.bfloat16)

    for phase, (low, top) in enumerate(phases):
        with jax.named_scope(f"recv{phase}"):
            wait_moved(phase, recv_sem, arriving)
        with jax.named_scope(f"slots{phase}"):
            heights = [
                min(-(-(TRUNC + 1 - slot * device_total) // 16) * 16, depth)
                for slot in range(low, top)
            ]
            values = jnp.concatenate(
                [coefficients(low + index, height) for index, height in enumerate(heights)],
                axis=0,
            )
            product = lax.dot_general(
                values, values, (((0,), (0,)), ((), ())), preferred_element_type=jnp.float32
            )
            gram_ref[...] = product if phase == 0 else gram_ref[...] + product

    gram = None
    for part in range(2):
        across = jnp.concatenate(
            [
                gram_ref[pl.ds(tm * LANES + part * HALF, months), :]
                for tm in range(tm_devices)
            ],
            axis=0,
        )
        block = jnp.concatenate(
            [
                across[:, tm * LANES + part * HALF : tm * LANES + part * HALF + months]
                for tm in range(tm_devices)
            ],
            axis=1,
        )
        gram = block if gram is None else gram + block
    on_diagonal = lax.broadcasted_iota(jnp.int32, gram.shape, 0) == lax.broadcasted_iota(
        jnp.int32, gram.shape, 1
    )
    diagonal = jnp.sum(jnp.where(on_diagonal, gram, 0.0), axis=0, keepdims=True)
    local_gram[:, :PIECE] = gram.reshape(pieces, PIECE, month_total)
    local_gram[:, PIECE:] = jnp.broadcast_to(diagonal[None], (pieces, 1, month_total))

    first_lat = lat_me // group * group
    place = lat_me % group
    local_me = place * tm_devices + tm_me

    def send_part(other, tm):
        return pltpu.make_async_remote_copy(
            src_ref=local_gram.at[tm * group + other],
            dst_ref=parts.at[local_me],
            send_sem=tail_sem.at[0],
            recv_sem=tail_sem.at[1],
            device_id=(first_lat + other, tm),
            device_id_type=MESH,
        )

    def send_sum(lat):
        return pltpu.make_async_remote_copy(
            src_ref=own_sum,
            dst_ref=full.at[lat_me],
            send_sem=tail_sem.at[2],
            recv_sem=tail_sem.at[3],
            device_id=(lat, tm_me),
            device_id_type=MESH,
        )

    def wait_tail(index, ref, count):
        if count:
            span = ref.at[pl.ds(0, count)]
            pltpu.make_async_copy(span, span, tail_sem.at[index]).wait()

    for other in range(group):
        for tm in range(tm_devices):

            @pl.when((other != place) | (tm != tm_me))
            def _():
                send_part(other, tm).start()

    with jax.named_scope("waitsend"):
        for phase in range(len(phases)):
            wait_moved(phase, send_sem, leaving)
        for source, via, counts in routes:

            @pl.when(lat_me == source)
            def _():
                wait_relay(0, relay)

            @pl.when(lat_me == via)
            def _():
                wait_blocks(
                    relay_sem.at[2], hemisphere * tm_devices * blocks_of(0, counts, True)
                )

    parts[local_me] = local_gram[tm_me * group + place]
    with jax.named_scope("owner"):
        wait_tail(1, parts, pieces - 1)
    total = jnp.sum(parts[...], axis=0)
    own_sum[...] = total
    full[lat_me] = total

    @pl.loop(1, lat_devices)
    def _(step):
        send_sum(lax.rem(lat_me + step, lat_devices)).start()

    with jax.named_scope("waitsum"):
        wait_tail(3, full, lat_devices - 1)

    with jax.named_scope("norm"):
        sums = full[:group]
        for block in range(group, lat_devices, group):
            sums = sums + full[block : block + group]
        trace = jnp.sum(sums[0, PIECE:])
        here = sums[:, :PIECE].reshape(months, month_total)
        out_ref[...] = month_total * here / (trace + 1e-06)

    with jax.named_scope("drain"):
        wait_tail(0, local_gram, pieces - 1)
        wait_tail(2, full, lat_devices - 1)


def solution(mesh):
    lat_devices = mesh.shape["lat"]
    tm_devices = mesh.shape["tm"]
    device_total = lat_devices * tm_devices
    slots = -(-(TRUNC + 1) // device_total)
    slot_rows = -(-slots // 8) * 8
    depth = -(-(TRUNC + 1) // 8) * 8

    def local(fields):
        rows, months, lon_count = fields.shape
        month_total = months * tm_devices
        lat_total = rows * lat_devices
        share = HALF // months
        high = rows // share
        pieces = month_total // PIECE
        width = tm_devices * LANES
        dims = (lat_devices, tm_devices, rows, months, lon_count, slots, slot_rows, depth)
        rank = ranks(lat_devices, tm_devices)
        table = jnp.asarray(twiddle_table(rank, slots, lon_count))
        starts = jnp.asarray(start_table(rank, slots, slot_rows))
        lats = jnp.asarray(lat_table(lat_total, share))
        bands = 2 if high % 16 == 0 else 1
        runs = needed_slots(lat_devices, device_total, slots, rows, bands)
        phases = phase_bounds(slots)
        longest = max(top - low for low, top in phases)
        routes = relay_routes(lat_devices, months // PIECE, runs, phases[0][1])
        carried = max([max(counts) * bands for source, via, counts in routes] + [1])
        hbm = pl.BlockSpec(memory_space=pl.ANY)
        vmem = pl.BlockSpec(memory_space=pltpu.VMEM)
        dma = pltpu.SemaphoreType.DMA
        return pl.pallas_call(
            functools.partial(kernel, dims, runs, routes),
            out_shape=pltpu.VMEM((months, month_total), jnp.float32),
            in_specs=[hbm, hbm, hbm, hbm],
            out_specs=vmem,
            scratch_shapes=[
                pltpu.VMEM((rows * months, lon_count), jnp.bfloat16),
                pltpu.VMEM(table.shape, jnp.bfloat16),
                pltpu.VMEM(starts.shape[1:], jnp.float32),
                pltpu.VMEM(lats.shape, jnp.float32),
                pltpu.VMEM((device_total * longest * high, LANES), jnp.float32),
                pltpu.VMEM((device_total, slots * bands, high // bands, LANES), jnp.bfloat16),
                pltpu.VMEM((device_total, slots * bands, high // bands, LANES), jnp.bfloat16),
                pltpu.VMEM((device_total // 2, carried, high // bands, LANES), jnp.bfloat16),
                pltpu.VMEM((lat_total // LANES, slot_rows * depth, LANES), jnp.float32),
                pltpu.VMEM((width, width), jnp.float32),
                pltpu.VMEM((pieces, PIECE + 1, month_total), jnp.float32),
                pltpu.VMEM((pieces, PIECE + 1, month_total), jnp.float32),
                pltpu.VMEM((PIECE + 1, month_total), jnp.float32),
                pltpu.VMEM((lat_devices, PIECE + 1, month_total), jnp.float32),
                dma,
                dma((len(phases),)),
                dma((2,)),
                dma((len(phases),)),
                dma((len(phases),)),
                dma((3,)),
                dma((4,)),
            ],
            compiler_params=pltpu.CompilerParams(
                collective_id=0, has_side_effects=True, vmem_limit_bytes=60 * 1024 * 1024
            ),
        )(fields.reshape(rows * months, lon_count), table, starts, lats)

    return jax.shard_map(
        local, mesh=mesh, in_specs=(P("lat", "tm", None),), out_specs=P("tm", None), check_vma=False
    )
```

```python
import functools
import math

import jax
import jax.numpy as jnp
import numpy as np
from jax import lax
from jax.experimental import pallas as pl
from jax.experimental.pallas import tpu as pltpu
from jax.sharding import PartitionSpec as P

TRUNC = 341
LANES = 128
HALF = 64
PIECE = 8
PHASES = 3
CHUNKS = 2
MESH = pl.DeviceIdType.MESH


def phase_bounds(slots):
    length = -(-slots // PHASES)
    return [(low, min(low + length, slots)) for low in range(0, slots, length)]


def rank_of(lat, tm, lat_devices, tm_devices):
    hemisphere = lat_devices // 2
    return ((lat % hemisphere) * tm_devices + tm) * 2 + lat // hemisphere


def ranks(lat_devices, tm_devices):
    device = np.arange(lat_devices * tm_devices)
    return rank_of(device // tm_devices, device % tm_devices, lat_devices, tm_devices)


def twiddle_table(rank, slots, lon_count):
    device_total = len(rank)
    longitude = np.arange(lon_count)
    parts = []
    for low, top in phase_bounds(slots):
        wave = (np.arange(low, top)[None, :] * device_total + rank[:, None]).reshape(-1, 1)
        phase = 2.0 * math.pi * ((wave * longitude) % lon_count) / lon_count
        active = (wave <= TRUNC) / math.sqrt(lon_count)
        parts += [np.cos(phase) * active, -np.sin(phase) * active]
    return np.concatenate(parts).astype(np.float32).astype(jnp.bfloat16)


def start_table(rank, slots, slot_rows):
    device_total = len(rank)
    table = np.zeros((device_total, slot_rows), np.float64)
    for device in range(device_total):
        for slot in range(slot_rows):
            order = min(slot, slots - 1) * device_total + int(rank[device])
            table[device, slot] = 0.5 * (
                math.log(0.5)
                + math.lgamma(order + 1.5)
                - math.lgamma(1.5)
                - math.lgamma(order + 1.0)
            )
    table = np.broadcast_to(table[:, :, None], (device_total, slot_rows, LANES))
    return table.astype(np.float32)


def needed_slots(lat_devices, device_total, slots, rows, bands):
    counts = []
    order = np.arange(slots * device_total)
    rise = np.array(
        [math.lgamma(m + 1.5) - math.lgamma(1.5) - math.lgamma(m + 1.0) for m in order]
    )
    for device in range(lat_devices):
        lat = device * rows + np.arange(rows)
        sine = np.sin(math.pi * (lat + 0.5) / (lat_devices * rows))
        start = 0.5 * (math.log(0.5) + rise[:, None]) + order[:, None] * np.log(sine)[None, :]
        used = (start > -70.5) & (order <= TRUNC)[:, None]
        used = used.reshape(slots, device_total, bands, -1).any(axis=(1, 3))
        counts.append(
            tuple(
                int(np.max(np.nonzero(used[:, band])[0])) + 1 if used[:, band].any() else 0
                for band in range(bands)
            )
        )
    runs = []
    for device, count in enumerate(counts):
        if runs and runs[-1][2] == count:
            runs[-1][1] = device + 1
        else:
            runs.append([device, device + 1, count])
    return tuple(tuple(run) for run in runs)


def relay_routes(lat_devices, group, runs, first_top):
    if lat_devices != 4 * group or group % 2:
        return ()
    routes = []
    for source, via in ((group // 2, 0), (lat_devices - 1 - group // 2, lat_devices - 1)):
        for first, last, counts in runs:
            if (first, last) == (source, source + 1) and 0 < max(counts) <= first_top:
                routes.append((source, via, counts))
    return tuple(routes)


def lat_table(lat_total, share):
    lat = np.arange(lat_total).reshape(lat_total // share, share).T.reshape(-1)
    theta = math.pi * (lat + 0.5) / lat_total
    table = np.stack([np.cos(theta), np.log(np.sin(theta)), math.pi * np.sin(theta) / lat_total])
    return table.reshape(3, lat_total // LANES, LANES).astype(np.float32)


def kernel(
    dims,
    runs,
    routes,
    x_hbm,
    table_hbm,
    start_hbm,
    lat_hbm,
    out_ref,
    x_ref,
    table_ref,
    start_ref,
    lat_ref,
    spread,
    outbox,
    inbox,
    relay,
    legendre,
    gram_ref,
    local_gram,
    parts,
    own_sum,
    full,
    x_sem,
    table_sem,
    small_sem,
    send_sem,
    recv_sem,
    far_sem,
    relay_sem,
    tail_sem,
):
    lat_devices, tm_devices, rows, months, lon_count, slots, slot_rows, depth = dims
    device_total = lat_devices * tm_devices
    share = HALF // months
    high = rows // share
    lat_total = lat_devices * rows
    lat_groups = lat_total // LANES
    month_total = months * tm_devices
    group = months // PIECE
    pieces = group * tm_devices
    lat_me = lax.axis_index("lat")
    tm_me = lax.axis_index("tm")
    me = lat_me * tm_devices + tm_me
    rank_me = rank_of(lat_me, tm_me, lat_devices, tm_devices)

    phases = phase_bounds(slots)

    def each_peer(act):
        def row(lat):
            for tm in range(tm_devices):
                act(lat, tm)

        pl.loop(lat_me + 1, lat_devices)(row)
        pl.loop(0, lat_me)(row)
        for tm in range(tm_devices):

            @pl.when(tm_me != tm)
            def _():
                act(lat_me, tm)

    barrier = pltpu.get_barrier_semaphore()
    staged = lat_devices == 4 * group and len(phase_bounds(slots)) > 1
    block_me = lat_me // group

    def near(lat):
        return jnp.abs(lat // group - block_me) <= 1

    def greet(lat, tm):
        def signal():
            pl.semaphore_signal(barrier, inc=1, device_id=(lat, tm), device_id_type=MESH)

        if staged:
            pl.when(near(lat))(signal)
        else:
            signal()

    each_peer(greet)

    def pass_on(index, block, other):
        @pl.when(block_me == block)
        def _():
            pl.semaphore_signal(
                far_sem.at[index],
                inc=1,
                device_id=(lat_me + (other - block) * group, tm_me),
                device_id_type=MESH,
            )

    def wait_near():
        if not staged:
            pl.semaphore_wait(barrier, device_total - 1)
            return
        inner = (block_me == 1) | (block_me == 2)
        size = group * tm_devices
        pl.when(inner)(lambda: pl.semaphore_wait(barrier, 3 * size - 1))
        pl.when(jnp.logical_not(inner))(lambda: pl.semaphore_wait(barrier, 2 * size - 1))
        for block, other in ((1, 0), (1, 2), (2, 1), (2, 3)):
            pass_on(0, block, other)

    def wait_far():
        pl.semaphore_wait(far_sem.at[0], 1)
        pass_on(1, 1, 0)
        pass_on(1, 2, 3)

        @pl.when((block_me == 0) | (block_me == 3))
        def _():
            pl.semaphore_wait(far_sem.at[1], 1)

    hemisphere = lat_devices // 2

    def each_target(act):
        @pl.loop(0, lat_devices)
        def _(step):
            if lat_devices & (lat_devices - 1):
                lat = lax.rem(lat_me + step, lat_devices)
            else:
                lat = lat_me ^ ((step // 2) ^ ((step + 1) % 2 * hemisphere))
            for tm in range(tm_devices):

                @pl.when((lat != lat_me) | (tm != tm_me))
                def _():
                    act(lat, tm)

    chunk = rows * months // CHUNKS

    def x_copy(index):
        span = pl.ds(index * chunk, chunk)
        return pltpu.make_async_copy(x_hbm.at[span], x_ref.at[span], x_sem.at[index])

    def table_copy(phase):
        low, top = phases[phase]
        span = pl.ds(2 * device_total * low, 2 * device_total * (top - low))
        return pltpu.make_async_copy(table_hbm.at[span], table_ref.at[span], table_sem.at[phase])

    table_copy(0).start()
    for index in range(CHUNKS):
        x_copy(index).start()

    start_copy = pltpu.make_async_copy(start_hbm.at[me], start_ref, small_sem.at[0])
    start_copy.start()
    lat_copy = pltpu.make_async_copy(lat_hbm, lat_ref, small_sem.at[1])
    lat_copy.start()

    bands = len(runs[0][2])
    band_rows = high // bands
    for first, last, counts in runs:
        for band, count in enumerate(counts):
            if count < slots:

                @pl.loop(first * tm_devices, last * tm_devices)
                def _(source):
                    for slot in range(count, slots):
                        inbox[source, slot * bands + band] = jnp.zeros(
                            (band_rows, LANES), jnp.bfloat16
                        )

    last_order = (slots - 1) * device_total
    last_holders = min(TRUNC + 1 - last_order, device_total)

    def holds_last(lat, tm):
        return last_order + rank_of(lat, tm, lat_devices, tm_devices) <= TRUNC

    def splits(phase):
        return phases[phase][1] == slots and last_holders < device_total

    if last_holders < device_total:

        @pl.when(jnp.logical_not(holds_last(lat_me, tm_me)))
        def _():
            inbox[:, (slots - 1) * bands :] = jnp.zeros(
                (device_total, bands, band_rows, LANES), jnp.bfloat16
            )

    def pieces_of(phase, counts, held):
        low, top = phases[phase]
        if not held:
            top = min(top, slots - 1)
        found = []
        shared = min(min(counts), top)
        if shared > low:
            found.append((low * bands, (shared - low) * bands))
        for band, count in enumerate(counts):
            for slot in range(max(low, min(counts)), min(count, top)):
                found.append((slot * bands + band, 1))
        return found

    def blocks_of(phase, counts, held):
        return sum(length for first, length in pieces_of(phase, counts, held))

    sources = [source for source, via, counts in routes]

    def relays(phase, first):
        return phase == 0 and first in sources

    def leaving(phase, first, counts, held):
        if relays(phase, first):
            return blocks_of(phase, counts, held) * (device_total // 2 - 1)
        kept = blocks_of(phase, counts, True) * last_holders
        rest = blocks_of(phase, counts, False) * (device_total - last_holders)
        return kept + rest - blocks_of(phase, counts, held)

    def arriving(phase, first, counts, held):
        total = sum(
            (last - first) * tm_devices * blocks_of(phase, counts, held)
            for first, last, counts in runs
        )
        return total - blocks_of(phase, counts, held)

    def each_case(phase, held, act):
        if splits(phase):
            pl.when(held)(lambda: act(True))
            pl.when(jnp.logical_not(held))(lambda: act(False))
        else:
            act(True)

    def wait_blocks(semaphore, count):
        if count:
            span = spread.at[pl.ds(0, count * band_rows // 2)]
            pltpu.make_async_copy(span, span, semaphore).wait()

    def each_class(act):
        for first, last, counts in runs:

            @pl.when((lat_me >= first) & (lat_me < last))
            def _():
                act(first, counts)

    def transform(phase):
        low, top = phases[phase]
        group_rows = device_total * (top - low)
        lower = lax.broadcasted_iota(jnp.int32, (group_rows, LANES), 1) < HALF
        table_copy(phase).wait()
        for index in range(CHUNKS):
            if phase == 0:
                x_copy(index).wait()
                if index == 0:
                    for later in range(1, len(phases)):
                        table_copy(later).start()
            values = lax.dot_general(
                table_ref[2 * device_total * low : 2 * device_total * top],
                x_ref[index * chunk : (index + 1) * chunk],
                (((1,), (1,)), ((), ())),
                preferred_element_type=jnp.float32,
            )
            for block in range(chunk // LANES):
                cosine = values[:group_rows, block * LANES : (block + 1) * LANES]
                sine = values[group_rows:, block * LANES : (block + 1) * LANES]
                even = jnp.where(lower, cosine, pltpu.roll(sine, HALF, 1))
                odd = jnp.where(lower, pltpu.roll(cosine, HALF, 1), sine)
                row = 2 * (index * chunk // LANES + block)
                spread[pl.ds(row, group_rows, stride=high), :] = even
                spread[pl.ds(row + 1, group_rows, stride=high), :] = odd
        packed = spread[: group_rows * high].astype(jnp.bfloat16)
        outbox[:, low * bands : top * bands] = packed.reshape(
            device_total, (top - low) * bands, band_rows, LANES
        )

    def exchange(phase, piece, lat, tm):
        span = pl.ds(*piece)
        return pltpu.make_async_remote_copy(
            src_ref=outbox.at[lat * tm_devices + tm, span],
            dst_ref=inbox.at[me, span],
            send_sem=send_sem.at[phase],
            recv_sem=recv_sem.at[phase],
            device_id=(lat, tm),
            device_id_type=MESH,
        )

    def across(source):
        return hemisphere - source // hemisphere * hemisphere

    def to_relay(source, via):
        span = pl.ds(across(source) * tm_devices, hemisphere * tm_devices)
        return pltpu.make_async_remote_copy(
            src_ref=outbox.at[span, pl.ds(0, relay.shape[1])],
            dst_ref=relay,
            send_sem=relay_sem.at[0],
            recv_sem=relay_sem.at[1],
            device_id=(via, tm_me),
            device_id_type=MESH,
        )

    def from_relay(source, counts):
        @pl.loop(0, hemisphere * tm_devices)
        def _(index):
            for piece in pieces_of(0, counts, True):
                span = pl.ds(*piece)
                pltpu.make_async_remote_copy(
                    src_ref=relay.at[index, span],
                    dst_ref=inbox.at[source * tm_devices + tm_me, span],
                    send_sem=relay_sem.at[2],
                    recv_sem=recv_sem.at[0],
                    device_id=(across(source) + index // tm_devices, index % tm_devices),
                    device_id_type=MESH,
                ).start()

    def send(phase, reach=None):
        def send_class(start, counts):
            def send_to(lat, tm):
                if reach is None:
                    send_one(lat, tm)
                else:
                    pl.when(near(lat) == reach)(lambda: send_one(lat, tm))

            def send_one(lat, tm):
                def go(held):
                    for piece in pieces_of(phase, counts, held):
                        exchange(phase, piece, lat, tm).start()

                each_case(phase, holds_last(lat, tm), go)

            def send_near(lat, tm):
                pl.when(lat // hemisphere == start // hemisphere)(lambda: send_to(lat, tm))

            if relays(phase, start) and reach is False:
                return
            if relays(phase, start):
                for source, via, _ in routes:
                    if source == start:
                        to_relay(source, via).start()
                each_target(send_near)
            elif pieces_of(phase, counts, True):
                each_target(send_to)

        each_class(send_class)

    held_here = holds_last(lat_me, tm_me)

    def wait_moved(phase, semaphore, amount):
        each_class(
            lambda first, counts: each_case(
                phase,
                held_here,
                lambda held: wait_blocks(semaphore.at[phase], amount(phase, first, counts, held)),
            )
        )

    for phase in range(len(phases)):
        with jax.named_scope(f"transform{phase}"):
            transform(phase)
        if phase == 0:
            with jax.named_scope("barrier"):
                wait_near()
        if phase == 1 and staged:
            with jax.named_scope("far"):
                wait_far()
            send(0, False)
        with jax.named_scope(f"send{phase}"):
            if phase == 0 and staged:
                send(0, True)
            else:
                send(phase)

    def wait_relay(index, ref):
        pltpu.make_async_copy(ref, ref, relay_sem.at[index]).wait()

    with jax.named_scope("relay"):
        for source, via, counts in routes:

            @pl.when(lat_me == via)
            def _():
                wait_relay(1, relay)
                from_relay(source, counts)

    inbox[me] = outbox[me]

    start_copy.wait()
    lat_copy.wait()

    halves = slot_rows // 8
    sub = lax.broadcasted_iota(jnp.int32, (8, LANES), 0)
    slot_of = [sub + 8 * half for half in range(halves)]
    order_int = [slot * device_total + rank_me for slot in slot_of]
    order = [value.astype(jnp.float32) for value in order_int]
    cosine_lat = [jnp.broadcast_to(lat_ref[0, pl.ds(g, 1), :], (8, LANES)) for g in range(lat_groups)]
    current = []
    scale = []
    for half in range(halves):
        factor = jnp.where(order_int[half] > 0, math.sqrt(2.0), 1.0)
        for g in range(lat_groups):
            log_start = (
                start_ref[pl.ds(8 * half, 8), :]
                + order[half] * jnp.broadcast_to(lat_ref[1, pl.ds(g, 1), :], (8, LANES))
            )
            taper = jnp.clip((log_start + 70.0) / 10.0, 0.0, 1.0)
            current.append(jnp.exp(jnp.maximum(log_start, -80.0)) * taper)
            scale.append(factor * jnp.broadcast_to(lat_ref[2, pl.ds(g, 1), :], (8, LANES)))

    def store(offset, values):
        for half in range(halves):
            keep = (order_int[half] + offset <= TRUNC) & (slot_of[half] < slots)
            for g in range(lat_groups):
                index = half * lat_groups + g
                value = jnp.where(keep, values[index] * scale[index], 0.0)
                legendre[g, pl.ds(8 * half * depth + offset, 8, stride=depth), :] = value

    store(0, current)

    def advance(offset, carry):
        now, before, backs = carry
        real = lax.convert_element_type(offset, jnp.float32)
        following = []
        next_backs = []
        for half in range(halves):
            degree = order[half] + real
            ratio = (4.0 * degree * degree - 1.0) / (real * (order[half] + degree))
            top = jnp.sqrt(ratio)
            next_backs.append(1.0 / top)
            for g in range(lat_groups):
                index = half * lat_groups + g
                following.append(
                    top * (cosine_lat[g] * now[index] - backs[half] * before[index])
                )
        store(offset, following)
        return following, now, next_backs

    zero = jnp.zeros((8, LANES), jnp.float32)
    with jax.named_scope("legendre"):
        lax.fori_loop(
            1,
            depth,
            advance,
            (current, [zero] * len(current), [zero] * halves),
            unroll=7,
        )

    per_share = lat_groups // share
    width = tm_devices * LANES

    def coefficients(slot, height):
        received = jnp.concatenate(
            [
                jnp.concatenate(
                    [
                        inbox[lat_device * tm_devices + tm, slot * bands : (slot + 1) * bands].reshape(
                            high, LANES
                        )
                        for lat_device in range(lat_devices)
                    ],
                    axis=0,
                )
                for tm in range(tm_devices)
            ],
            axis=1,
        )
        share_of = lax.broadcasted_iota(jnp.int32, (height, width), 1) % HALF // months
        first = slot * depth
        merged = None
        for part in range(share):
            basis = jnp.concatenate(
                [
                    legendre[part * per_share + g, first : first + height, :].astype(jnp.bfloat16)
                    for g in range(per_share)
                ],
                axis=1,
            )
            product = jnp.dot(basis, received, preferred_element_type=jnp.float32)
            merged = product if part == 0 else jnp.where(share_of == part, product, merged)
        total = merged
        for part in range(1, share):
            total = total + pltpu.roll(merged, width - part * months, 1)
        return jnp.where(share_of == 0, total, 0.0).astype(jnp.bfloat16)

    for phase, (low, top) in enumerate(phases):
        with jax.named_scope(f"recv{phase}"):
            wait_moved(phase, recv_sem, arriving)
        with jax.named_scope(f"slots{phase}"):
            heights = [
                min(-(-(TRUNC + 1 - slot * device_total) // 16) * 16, depth)
                for slot in range(low, top)
            ]
            values = jnp.concatenate(
                [coefficients(low + index, height) for index, height in enumerate(heights)],
                axis=0,
            )
            product = lax.dot_general(
                values, values, (((0,), (0,)), ((), ())), preferred_element_type=jnp.float32
            )
            gram_ref[...] = product if phase == 0 else gram_ref[...] + product

    gram = None
    for part in range(2):
        across = jnp.concatenate(
            [
                gram_ref[pl.ds(tm * LANES + part * HALF, months), :]
                for tm in range(tm_devices)
            ],
            axis=0,
        )
        block = jnp.concatenate(
            [
                across[:, tm * LANES + part * HALF : tm * LANES + part * HALF + months]
                for tm in range(tm_devices)
            ],
            axis=1,
        )
        gram = block if gram is None else gram + block
    on_diagonal = lax.broadcasted_iota(jnp.int32, gram.shape, 0) == lax.broadcasted_iota(
        jnp.int32, gram.shape, 1
    )
    diagonal = jnp.sum(jnp.where(on_diagonal, gram, 0.0), axis=0, keepdims=True)
    local_gram[:, :PIECE] = gram.reshape(pieces, PIECE, month_total)
    local_gram[:, PIECE:] = jnp.broadcast_to(diagonal[None], (pieces, 1, month_total))

    first_lat = lat_me // group * group
    place = lat_me % group
    local_me = place * tm_devices + tm_me

    def send_part(other, tm):
        return pltpu.make_async_remote_copy(
            src_ref=local_gram.at[tm * group + other],
            dst_ref=parts.at[local_me],
            send_sem=tail_sem.at[0],
            recv_sem=tail_sem.at[1],
            device_id=(first_lat + other, tm),
            device_id_type=MESH,
        )

    def send_sum(lat):
        return pltpu.make_async_remote_copy(
            src_ref=own_sum,
            dst_ref=full.at[lat_me],
            send_sem=tail_sem.at[2],
            recv_sem=tail_sem.at[3],
            device_id=(lat, tm_me),
            device_id_type=MESH,
        )

    def wait_tail(index, ref, count):
        if count:
            span = ref.at[pl.ds(0, count)]
            pltpu.make_async_copy(span, span, tail_sem.at[index]).wait()

    for other in range(group):
        for tm in range(tm_devices):

            @pl.when((other != place) | (tm != tm_me))
            def _():
                send_part(other, tm).start()

    with jax.named_scope("waitsend"):
        for phase in range(len(phases)):
            wait_moved(phase, send_sem, leaving)
        for source, via, counts in routes:

            @pl.when(lat_me == source)
            def _():
                wait_relay(0, relay)

            @pl.when(lat_me == via)
            def _():
                wait_blocks(
                    relay_sem.at[2], hemisphere * tm_devices * blocks_of(0, counts, True)
                )

    parts[local_me] = local_gram[tm_me * group + place]
    with jax.named_scope("owner"):
        wait_tail(1, parts, pieces - 1)
    total = jnp.sum(parts[...], axis=0)
    own_sum[...] = total
    full[lat_me] = total

    @pl.loop(1, lat_devices)
    def _(step):
        send_sum(lax.rem(lat_me + step, lat_devices)).start()

    with jax.named_scope("waitsum"):
        wait_tail(3, full, lat_devices - 1)

    with jax.named_scope("norm"):
        sums = full[:group]
        for block in range(group, lat_devices, group):
            sums = sums + full[block : block + group]
        trace = jnp.sum(sums[0, PIECE:])
        here = sums[:, :PIECE].reshape(months, month_total)
        out_ref[...] = month_total * here / (trace + 1e-06)

    with jax.named_scope("drain"):
        wait_tail(0, local_gram, pieces - 1)
        wait_tail(2, full, lat_devices - 1)


def solution(mesh):
    lat_devices = mesh.shape["lat"]
    tm_devices = mesh.shape["tm"]
    device_total = lat_devices * tm_devices
    slots = -(-(TRUNC + 1) // device_total)
    slot_rows = -(-slots // 8) * 8
    depth = -(-(TRUNC + 1) // 8) * 8

    def local(fields):
        rows, months, lon_count = fields.shape
        month_total = months * tm_devices
        lat_total = rows * lat_devices
        share = HALF // months
        high = rows // share
        pieces = month_total // PIECE
        width = tm_devices * LANES
        dims = (lat_devices, tm_devices, rows, months, lon_count, slots, slot_rows, depth)
        rank = ranks(lat_devices, tm_devices)
        table = jnp.asarray(twiddle_table(rank, slots, lon_count))
        starts = jnp.asarray(start_table(rank, slots, slot_rows))
        lats = jnp.asarray(lat_table(lat_total, share))
        bands = 2 if high % 16 == 0 else 1
        runs = needed_slots(lat_devices, device_total, slots, rows, bands)
        phases = phase_bounds(slots)
        longest = max(top - low for low, top in phases)
        routes = relay_routes(lat_devices, months // PIECE, runs, phases[0][1])
        carried = max([max(counts) * bands for source, via, counts in routes] + [1])
        hbm = pl.BlockSpec(memory_space=pl.ANY)
        vmem = pl.BlockSpec(memory_space=pltpu.VMEM)
        dma = pltpu.SemaphoreType.DMA
        return pl.pallas_call(
            functools.partial(kernel, dims, runs, routes),
            out_shape=pltpu.VMEM((months, month_total), jnp.float32),
            in_specs=[hbm, hbm, hbm, hbm],
            out_specs=vmem,
            scratch_shapes=[
                pltpu.VMEM((rows * months, lon_count), jnp.bfloat16),
                pltpu.VMEM(table.shape, jnp.bfloat16),
                pltpu.VMEM(starts.shape[1:], jnp.float32),
                pltpu.VMEM(lats.shape, jnp.float32),
                pltpu.VMEM((device_total * longest * high, LANES), jnp.float32),
                pltpu.VMEM((device_total, slots * bands, high // bands, LANES), jnp.bfloat16),
                pltpu.VMEM((device_total, slots * bands, high // bands, LANES), jnp.bfloat16),
                pltpu.VMEM((device_total // 2, carried, high // bands, LANES), jnp.bfloat16),
                pltpu.VMEM((lat_total // LANES, slot_rows * depth, LANES), jnp.float32),
                pltpu.VMEM((width, width), jnp.float32),
                pltpu.VMEM((pieces, PIECE + 1, month_total), jnp.float32),
                pltpu.VMEM((pieces, PIECE + 1, month_total), jnp.float32),
                pltpu.VMEM((PIECE + 1, month_total), jnp.float32),
                pltpu.VMEM((lat_devices, PIECE + 1, month_total), jnp.float32),
                dma((CHUNKS,)),
                dma((len(phases),)),
                dma((2,)),
                dma((len(phases),)),
                dma((len(phases),)),
                pltpu.SemaphoreType.REGULAR((2,)),
                dma((3,)),
                dma((4,)),
            ],
            compiler_params=pltpu.CompilerParams(
                collective_id=0, has_side_effects=True, vmem_limit_bytes=60 * 1024 * 1024
            ),
        )(fields.reshape(rows * months, lon_count), table, starts, lats)

    return jax.shard_map(
        local, mesh=mesh, in_specs=(P("lat", "tm", None),), out_specs=P("tm", None), check_vma=False
    )
```

```python
import functools
import math

import jax
import jax.numpy as jnp
import numpy as np
from jax import lax
from jax.experimental import pallas as pl
from jax.experimental.pallas import tpu as pltpu
from jax.sharding import PartitionSpec as P

TRUNC = 341
LANES = 128
HALF = 64
PIECE = 8
PHASES = 3
CHUNKS = 2
MESH = pl.DeviceIdType.MESH


def phase_bounds(slots):
    length = -(-slots // PHASES)
    return [(low, min(low + length, slots)) for low in range(0, slots, length)]


def rank_of(lat, tm, lat_devices, tm_devices):
    hemisphere = lat_devices // 2
    return ((lat % hemisphere) * tm_devices + tm) * 2 + lat // hemisphere


def ranks(lat_devices, tm_devices):
    device = np.arange(lat_devices * tm_devices)
    return rank_of(device // tm_devices, device % tm_devices, lat_devices, tm_devices)


def twiddle_table(rank, slots, lon_count):
    device_total = len(rank)
    longitude = np.arange(lon_count)
    parts = []
    for low, top in phase_bounds(slots):
        wave = (np.arange(low, top)[None, :] * device_total + rank[:, None]).reshape(-1, 1)
        phase = 2.0 * math.pi * ((wave * longitude) % lon_count) / lon_count
        active = (wave <= TRUNC) / math.sqrt(lon_count)
        parts += [np.cos(phase) * active, -np.sin(phase) * active]
    return np.concatenate(parts).astype(np.float32).astype(jnp.bfloat16)


def start_table(rank, slots, slot_rows):
    device_total = len(rank)
    table = np.zeros((device_total, slot_rows), np.float64)
    for device in range(device_total):
        for slot in range(slot_rows):
            order = min(slot, slots - 1) * device_total + int(rank[device])
            table[device, slot] = 0.5 * (
                math.log(0.5)
                + math.lgamma(order + 1.5)
                - math.lgamma(1.5)
                - math.lgamma(order + 1.0)
            )
    table = np.broadcast_to(table[:, :, None], (device_total, slot_rows, LANES))
    return table.astype(np.float32)


def needed_slots(lat_devices, device_total, slots, rows, bands):
    counts = []
    order = np.arange(slots * device_total)
    rise = np.array(
        [math.lgamma(m + 1.5) - math.lgamma(1.5) - math.lgamma(m + 1.0) for m in order]
    )
    for device in range(lat_devices):
        lat = device * rows + np.arange(rows)
        sine = np.sin(math.pi * (lat + 0.5) / (lat_devices * rows))
        start = 0.5 * (math.log(0.5) + rise[:, None]) + order[:, None] * np.log(sine)[None, :]
        used = (start > -70.5) & (order <= TRUNC)[:, None]
        used = used.reshape(slots, device_total, bands, -1).any(axis=(1, 3))
        counts.append(
            tuple(
                int(np.max(np.nonzero(used[:, band])[0])) + 1 if used[:, band].any() else 0
                for band in range(bands)
            )
        )
    runs = []
    for device, count in enumerate(counts):
        if runs and runs[-1][2] == count:
            runs[-1][1] = device + 1
        else:
            runs.append([device, device + 1, count])
    return tuple(tuple(run) for run in runs)


def relay_routes(lat_devices, group, runs, first_top):
    if lat_devices != 4 * group or group % 2:
        return ()
    routes = []
    for source, via in ((group // 2, 0), (lat_devices - 1 - group // 2, lat_devices - 1)):
        for first, last, counts in runs:
            if (first, last) == (source, source + 1) and 0 < max(counts) <= first_top:
                routes.append((source, via, counts))
    return tuple(routes)


def lat_table(lat_total, share):
    lat = np.arange(lat_total).reshape(lat_total // share, share).T.reshape(-1)
    theta = math.pi * (lat + 0.5) / lat_total
    table = np.stack([np.cos(theta), np.log(np.sin(theta)), math.pi * np.sin(theta) / lat_total])
    return table.reshape(3, lat_total // LANES, LANES).astype(np.float32)


def kernel(
    dims,
    runs,
    routes,
    x_hbm,
    table_hbm,
    start_hbm,
    lat_hbm,
    out_ref,
    x_ref,
    table_ref,
    start_ref,
    lat_ref,
    spread,
    outbox,
    inbox,
    relay,
    legendre,
    gram_ref,
    local_gram,
    parts,
    own_sum,
    full,
    x_sem,
    table_sem,
    small_sem,
    send_sem,
    recv_sem,
    far_sem,
    relay_sem,
    tail_sem,
):
    lat_devices, tm_devices, rows, months, lon_count, slots, slot_rows, depth = dims
    device_total = lat_devices * tm_devices
    share = HALF // months
    high = rows // share
    lat_total = lat_devices * rows
    lat_groups = lat_total // LANES
    month_total = months * tm_devices
    group = months // PIECE
    pieces = group * tm_devices
    lat_me = lax.axis_index("lat")
    tm_me = lax.axis_index("tm")
    me = lat_me * tm_devices + tm_me
    rank_me = rank_of(lat_me, tm_me, lat_devices, tm_devices)

    phases = phase_bounds(slots)

    def each_peer(act):
        def row(lat):
            for tm in range(tm_devices):
                act(lat, tm)

        pl.loop(lat_me + 1, lat_devices)(row)
        pl.loop(0, lat_me)(row)
        for tm in range(tm_devices):

            @pl.when(tm_me != tm)
            def _():
                act(lat_me, tm)

    barrier = pltpu.get_barrier_semaphore()
    staged = lat_devices == 4 * group and len(phase_bounds(slots)) > 1
    block_me = lat_me // group

    def near(lat):
        return jnp.abs(lat // group - block_me) <= 1

    def greet(lat, tm):
        def signal():
            pl.semaphore_signal(barrier, inc=1, device_id=(lat, tm), device_id_type=MESH)

        if staged:
            pl.when(near(lat))(signal)
        else:
            signal()

    each_peer(greet)

    def pass_on(index, block, other):
        @pl.when(block_me == block)
        def _():
            pl.semaphore_signal(
                far_sem.at[index],
                inc=1,
                device_id=(lat_me + (other - block) * group, tm_me),
                device_id_type=MESH,
            )

    def wait_near():
        if not staged:
            pl.semaphore_wait(barrier, device_total - 1)
            return
        inner = (block_me == 1) | (block_me == 2)
        size = group * tm_devices
        pl.when(inner)(lambda: pl.semaphore_wait(barrier, 3 * size - 1))
        pl.when(jnp.logical_not(inner))(lambda: pl.semaphore_wait(barrier, 2 * size - 1))
        for block, other in ((1, 0), (1, 2), (2, 1), (2, 3)):
            pass_on(0, block, other)

    def wait_far():
        pl.semaphore_wait(far_sem.at[0], 1)
        pass_on(1, 1, 0)
        pass_on(1, 2, 3)

        @pl.when((block_me == 0) | (block_me == 3))
        def _():
            pl.semaphore_wait(far_sem.at[1], 1)

    hemisphere = lat_devices // 2

    def each_target(act):
        @pl.loop(0, lat_devices)
        def _(step):
            if lat_devices & (lat_devices - 1):
                lat = lax.rem(lat_me + step, lat_devices)
            else:
                lat = lat_me ^ ((step // 2) ^ ((step + 1) % 2 * hemisphere))
            for tm in range(tm_devices):

                @pl.when((lat != lat_me) | (tm != tm_me))
                def _():
                    act(lat, tm)

    chunk = rows * months // CHUNKS

    def x_copy(index):
        span = pl.ds(index * chunk, chunk)
        return pltpu.make_async_copy(x_hbm.at[span], x_ref.at[span], x_sem.at[index])

    def table_copy(phase):
        low, top = phases[phase]
        span = pl.ds(2 * device_total * low, 2 * device_total * (top - low))
        return pltpu.make_async_copy(table_hbm.at[span], table_ref.at[span], table_sem.at[phase])

    table_copy(0).start()
    for index in range(CHUNKS):
        x_copy(index).start()

    start_copy = pltpu.make_async_copy(start_hbm.at[me], start_ref, small_sem.at[0])
    start_copy.start()
    lat_copy = pltpu.make_async_copy(lat_hbm, lat_ref, small_sem.at[1])
    lat_copy.start()

    bands = len(runs[0][2])
    band_rows = high // bands
    for first, last, counts in runs:
        for band, count in enumerate(counts):
            if count < slots:

                @pl.loop(first * tm_devices, last * tm_devices)
                def _(source):
                    for slot in range(count, slots):
                        inbox[source, slot * bands + band] = jnp.zeros(
                            (band_rows, LANES), jnp.bfloat16
                        )

    last_order = (slots - 1) * device_total
    last_holders = min(TRUNC + 1 - last_order, device_total)

    def holds_last(lat, tm):
        return last_order + rank_of(lat, tm, lat_devices, tm_devices) <= TRUNC

    def splits(phase):
        return phases[phase][1] == slots and last_holders < device_total

    if last_holders < device_total:

        @pl.when(jnp.logical_not(holds_last(lat_me, tm_me)))
        def _():
            inbox[:, (slots - 1) * bands :] = jnp.zeros(
                (device_total, bands, band_rows, LANES), jnp.bfloat16
            )

    def pieces_of(phase, counts, held):
        low, top = phases[phase]
        if not held:
            top = min(top, slots - 1)
        found = []
        shared = min(min(counts), top)
        if shared > low:
            found.append((low * bands, (shared - low) * bands))
        for band, count in enumerate(counts):
            for slot in range(max(low, min(counts)), min(count, top)):
                found.append((slot * bands + band, 1))
        return found

    def blocks_of(phase, counts, held):
        return sum(length for first, length in pieces_of(phase, counts, held))

    sources = [source for source, via, counts in routes]

    def relays(phase, first):
        return phase == 0 and first in sources

    def leaving(phase, first, counts, held):
        if relays(phase, first):
            return blocks_of(phase, counts, held) * (device_total // 2 - 1)
        kept = blocks_of(phase, counts, True) * last_holders
        rest = blocks_of(phase, counts, False) * (device_total - last_holders)
        return kept + rest - blocks_of(phase, counts, held)

    def arriving(phase, first, counts, held):
        total = sum(
            (last - first) * tm_devices * blocks_of(phase, counts, held)
            for first, last, counts in runs
        )
        return total - blocks_of(phase, counts, held)

    def each_case(phase, held, act):
        if splits(phase):
            pl.when(held)(lambda: act(True))
            pl.when(jnp.logical_not(held))(lambda: act(False))
        else:
            act(True)

    def wait_blocks(semaphore, count):
        if count:
            span = spread.at[pl.ds(0, count * band_rows // 2)]
            pltpu.make_async_copy(span, span, semaphore).wait()

    def each_class(act):
        for first, last, counts in runs:

            @pl.when((lat_me >= first) & (lat_me < last))
            def _():
                act(first, counts)

    def transform(phase):
        low, top = phases[phase]
        group_rows = device_total * (top - low)
        lower = lax.broadcasted_iota(jnp.int32, (group_rows, LANES), 1) < HALF
        table_copy(phase).wait()
        for index in range(CHUNKS):
            if phase == 0:
                x_copy(index).wait()
                if index == 0:
                    for later in range(1, len(phases)):
                        table_copy(later).start()
            values = lax.dot_general(
                table_ref[2 * device_total * low : 2 * device_total * top],
                x_ref[index * chunk : (index + 1) * chunk],
                (((1,), (1,)), ((), ())),
                preferred_element_type=jnp.float32,
            )
            for block in range(chunk // LANES):
                cosine = values[:group_rows, block * LANES : (block + 1) * LANES]
                sine = values[group_rows:, block * LANES : (block + 1) * LANES]
                even = jnp.where(lower, cosine, pltpu.roll(sine, HALF, 1))
                odd = jnp.where(lower, pltpu.roll(cosine, HALF, 1), sine)
                row = 2 * (index * chunk // LANES + block)
                spread[pl.ds(row, group_rows, stride=high), :] = even
                spread[pl.ds(row + 1, group_rows, stride=high), :] = odd
        packed = spread[: group_rows * high].astype(jnp.bfloat16)
        outbox[:, low * bands : top * bands] = packed.reshape(
            device_total, (top - low) * bands, band_rows, LANES
        )

    def exchange(phase, piece, lat, tm):
        span = pl.ds(*piece)
        return pltpu.make_async_remote_copy(
            src_ref=outbox.at[lat * tm_devices + tm, span],
            dst_ref=inbox.at[me, span],
            send_sem=send_sem.at[phase],
            recv_sem=recv_sem.at[phase],
            device_id=(lat, tm),
            device_id_type=MESH,
        )

    def across(source):
        return hemisphere - source // hemisphere * hemisphere

    def to_relay(source, via):
        span = pl.ds(across(source) * tm_devices, hemisphere * tm_devices)
        return pltpu.make_async_remote_copy(
            src_ref=outbox.at[span, pl.ds(0, relay.shape[1])],
            dst_ref=relay,
            send_sem=relay_sem.at[0],
            recv_sem=relay_sem.at[1],
            device_id=(via, tm_me),
            device_id_type=MESH,
        )

    def from_relay(source, counts):
        @pl.loop(0, hemisphere * tm_devices)
        def _(index):
            for piece in pieces_of(0, counts, True):
                span = pl.ds(*piece)
                pltpu.make_async_remote_copy(
                    src_ref=relay.at[index, span],
                    dst_ref=inbox.at[source * tm_devices + tm_me, span],
                    send_sem=relay_sem.at[2],
                    recv_sem=recv_sem.at[0],
                    device_id=(across(source) + index // tm_devices, index % tm_devices),
                    device_id_type=MESH,
                ).start()

    def send(phase, reach=None):
        def send_class(start, counts):
            def send_to(lat, tm):
                if reach is None:
                    send_one(lat, tm)
                else:
                    pl.when(near(lat) == reach)(lambda: send_one(lat, tm))

            def send_one(lat, tm):
                def go(held):
                    for piece in pieces_of(phase, counts, held):
                        exchange(phase, piece, lat, tm).start()

                each_case(phase, holds_last(lat, tm), go)

            def send_near(lat, tm):
                pl.when(lat // hemisphere == start // hemisphere)(lambda: send_to(lat, tm))

            if relays(phase, start) and reach is False:
                return
            if relays(phase, start):
                for source, via, _ in routes:
                    if source == start:
                        to_relay(source, via).start()
                each_target(send_near)
            elif pieces_of(phase, counts, True):
                each_target(send_to)

        each_class(send_class)

    held_here = holds_last(lat_me, tm_me)

    def wait_moved(phase, semaphore, amount):
        each_class(
            lambda first, counts: each_case(
                phase,
                held_here,
                lambda held: wait_blocks(semaphore.at[phase], amount(phase, first, counts, held)),
            )
        )

    for phase in range(len(phases)):
        with jax.named_scope(f"transform{phase}"):
            transform(phase)
        if phase == 0:
            with jax.named_scope("barrier"):
                wait_near()
        if phase == 1 and staged:
            with jax.named_scope("far"):
                wait_far()
            send(0, False)
        with jax.named_scope(f"send{phase}"):
            if phase == 0 and staged:
                send(0, True)
            else:
                send(phase)

    def wait_relay(index, ref):
        pltpu.make_async_copy(ref, ref, relay_sem.at[index]).wait()

    with jax.named_scope("relay"):
        for source, via, counts in routes:

            @pl.when(lat_me == via)
            def _():
                wait_relay(1, relay)
                from_relay(source, counts)

    inbox[me] = outbox[me]

    start_copy.wait()
    lat_copy.wait()

    halves = slot_rows // 8
    sub = lax.broadcasted_iota(jnp.int32, (8, LANES), 0)
    slot_of = [sub + 8 * half for half in range(halves)]
    order_int = [slot * device_total + rank_me for slot in slot_of]
    order = [value.astype(jnp.float32) for value in order_int]
    cosine_lat = [jnp.broadcast_to(lat_ref[0, pl.ds(g, 1), :], (8, LANES)) for g in range(lat_groups)]
    current = []
    scale = []
    for half in range(halves):
        factor = jnp.where(order_int[half] > 0, math.sqrt(2.0), 1.0)
        for g in range(lat_groups):
            log_start = (
                start_ref[pl.ds(8 * half, 8), :]
                + order[half] * jnp.broadcast_to(lat_ref[1, pl.ds(g, 1), :], (8, LANES))
            )
            taper = jnp.clip((log_start + 70.0) / 10.0, 0.0, 1.0)
            current.append(jnp.exp(jnp.maximum(log_start, -80.0)) * taper)
            scale.append(factor * jnp.broadcast_to(lat_ref[2, pl.ds(g, 1), :], (8, LANES)))

    def store(offset, values):
        for half in range(halves):
            keep = (order_int[half] + offset <= TRUNC) & (slot_of[half] < slots)
            for g in range(lat_groups):
                index = half * lat_groups + g
                value = jnp.where(keep, values[index] * scale[index], 0.0)
                legendre[g, pl.ds(8 * half * depth + offset, 8, stride=depth), :] = value

    store(0, current)

    def advance(offset, carry):
        now, before, backs = carry
        real = lax.convert_element_type(offset, jnp.float32)
        following = []
        next_backs = []
        for half in range(halves):
            degree = order[half] + real
            ratio = (4.0 * degree * degree - 1.0) / (real * (order[half] + degree))
            top = jnp.sqrt(ratio)
            next_backs.append(1.0 / top)
            for g in range(lat_groups):
                index = half * lat_groups + g
                following.append(
                    top * (cosine_lat[g] * now[index] - backs[half] * before[index])
                )
        store(offset, following)
        return following, now, next_backs

    zero = jnp.zeros((8, LANES), jnp.float32)
    with jax.named_scope("legendre"):
        lax.fori_loop(
            1,
            depth,
            advance,
            (current, [zero] * len(current), [zero] * halves),
            unroll=7,
        )

    per_share = lat_groups // share
    width = tm_devices * LANES

    def coefficients(slot, height):
        received = jnp.concatenate(
            [
                jnp.concatenate(
                    [
                        inbox[lat_device * tm_devices + tm, slot * bands : (slot + 1) * bands].reshape(
                            high, LANES
                        )
                        for lat_device in range(lat_devices)
                    ],
                    axis=0,
                )
                for tm in range(tm_devices)
            ],
            axis=1,
        )
        share_of = lax.broadcasted_iota(jnp.int32, (height, width), 1) % HALF // months
        first = slot * depth
        basis = jnp.concatenate(
            [
                jnp.concatenate(
                    [
                        legendre[part * per_share + g, first : first + height, :]
                        for g in range(per_share)
                    ],
                    axis=1,
                )
                for part in range(share)
            ],
            axis=0,
        ).astype(jnp.bfloat16)
        product = jnp.dot(basis, received, preferred_element_type=jnp.float32)
        merged = product[:height]
        for part in range(1, share):
            part_product = product[part * height : (part + 1) * height]
            merged = jnp.where(share_of == part, part_product, merged)
        total = merged
        for part in range(1, share):
            total = total + pltpu.roll(merged, width - part * months, 1)
        return jnp.where(share_of == 0, total, 0.0).astype(jnp.bfloat16)

    for phase, (low, top) in enumerate(phases):
        with jax.named_scope(f"recv{phase}"):
            wait_moved(phase, recv_sem, arriving)
        with jax.named_scope(f"slots{phase}"):
            heights = [
                min(-(-(TRUNC + 1 - slot * device_total) // 16) * 16, depth)
                for slot in range(low, top)
            ]
            values = jnp.concatenate(
                [coefficients(low + index, height) for index, height in enumerate(heights)],
                axis=0,
            )
            product = lax.dot_general(
                values, values, (((0,), (0,)), ((), ())), preferred_element_type=jnp.float32
            )
            gram_ref[...] = product if phase == 0 else gram_ref[...] + product

    gram = None
    for part in range(2):
        across = jnp.concatenate(
            [
                gram_ref[pl.ds(tm * LANES + part * HALF, months), :]
                for tm in range(tm_devices)
            ],
            axis=0,
        )
        block = jnp.concatenate(
            [
                across[:, tm * LANES + part * HALF : tm * LANES + part * HALF + months]
                for tm in range(tm_devices)
            ],
            axis=1,
        )
        gram = block if gram is None else gram + block
    on_diagonal = lax.broadcasted_iota(jnp.int32, gram.shape, 0) == lax.broadcasted_iota(
        jnp.int32, gram.shape, 1
    )
    diagonal = jnp.sum(jnp.where(on_diagonal, gram, 0.0), axis=0, keepdims=True)
    local_gram[:, :PIECE] = gram.reshape(pieces, PIECE, month_total)
    local_gram[:, PIECE:] = jnp.broadcast_to(diagonal[None], (pieces, 1, month_total))

    first_lat = lat_me // group * group
    place = lat_me % group
    local_me = place * tm_devices + tm_me

    def send_part(other, tm):
        return pltpu.make_async_remote_copy(
            src_ref=local_gram.at[tm * group + other],
            dst_ref=parts.at[local_me],
            send_sem=tail_sem.at[0],
            recv_sem=tail_sem.at[1],
            device_id=(first_lat + other, tm),
            device_id_type=MESH,
        )

    def send_sum(lat):
        return pltpu.make_async_remote_copy(
            src_ref=own_sum,
            dst_ref=full.at[lat_me],
            send_sem=tail_sem.at[2],
            recv_sem=tail_sem.at[3],
            device_id=(lat, tm_me),
            device_id_type=MESH,
        )

    def wait_tail(index, ref, count):
        if count:
            span = ref.at[pl.ds(0, count)]
            pltpu.make_async_copy(span, span, tail_sem.at[index]).wait()

    for other in range(group):
        for tm in range(tm_devices):

            @pl.when((other != place) | (tm != tm_me))
            def _():
                send_part(other, tm).start()

    with jax.named_scope("waitsend"):
        for phase in range(len(phases)):
            wait_moved(phase, send_sem, leaving)
        for source, via, counts in routes:

            @pl.when(lat_me == source)
            def _():
                wait_relay(0, relay)

            @pl.when(lat_me == via)
            def _():
                wait_blocks(
                    relay_sem.at[2], hemisphere * tm_devices * blocks_of(0, counts, True)
                )

    parts[local_me] = local_gram[tm_me * group + place]
    with jax.named_scope("owner"):
        wait_tail(1, parts, pieces - 1)
    total = jnp.sum(parts[...], axis=0)
    own_sum[...] = total
    full[lat_me] = total

    @pl.loop(1, lat_devices)
    def _(step):
        send_sum(lax.rem(lat_me + step, lat_devices)).start()

    with jax.named_scope("waitsum"):
        wait_tail(3, full, lat_devices - 1)

    with jax.named_scope("norm"):
        sums = full[:group]
        for block in range(group, lat_devices, group):
            sums = sums + full[block : block + group]
        trace = jnp.sum(sums[0, PIECE:])
        here = sums[:, :PIECE].reshape(months, month_total)
        out_ref[...] = month_total * here / (trace + 1e-06)

    with jax.named_scope("drain"):
        wait_tail(0, local_gram, pieces - 1)
        wait_tail(2, full, lat_devices - 1)


def solution(mesh):
    lat_devices = mesh.shape["lat"]
    tm_devices = mesh.shape["tm"]
    device_total = lat_devices * tm_devices
    slots = -(-(TRUNC + 1) // device_total)
    slot_rows = -(-slots // 8) * 8
    depth = -(-(TRUNC + 1) // 8) * 8

    def local(fields):
        rows, months, lon_count = fields.shape
        month_total = months * tm_devices
        lat_total = rows * lat_devices
        share = HALF // months
        high = rows // share
        pieces = month_total // PIECE
        width = tm_devices * LANES
        dims = (lat_devices, tm_devices, rows, months, lon_count, slots, slot_rows, depth)
        rank = ranks(lat_devices, tm_devices)
        table = jnp.asarray(twiddle_table(rank, slots, lon_count))
        starts = jnp.asarray(start_table(rank, slots, slot_rows))
        lats = jnp.asarray(lat_table(lat_total, share))
        bands = 2 if high % 16 == 0 else 1
        runs = needed_slots(lat_devices, device_total, slots, rows, bands)
        phases = phase_bounds(slots)
        longest = max(top - low for low, top in phases)
        routes = relay_routes(lat_devices, months // PIECE, runs, phases[0][1])
        carried = max([max(counts) * bands for source, via, counts in routes] + [1])
        hbm = pl.BlockSpec(memory_space=pl.ANY)
        vmem = pl.BlockSpec(memory_space=pltpu.VMEM)
        dma = pltpu.SemaphoreType.DMA
        return pl.pallas_call(
            functools.partial(kernel, dims, runs, routes),
            out_shape=pltpu.VMEM((months, month_total), jnp.float32),
            in_specs=[hbm, hbm, hbm, hbm],
            out_specs=vmem,
            scratch_shapes=[
                pltpu.VMEM((rows * months, lon_count), jnp.bfloat16),
                pltpu.VMEM(table.shape, jnp.bfloat16),
                pltpu.VMEM(starts.shape[1:], jnp.float32),
                pltpu.VMEM(lats.shape, jnp.float32),
                pltpu.VMEM((device_total * longest * high, LANES), jnp.float32),
                pltpu.VMEM((device_total, slots * bands, high // bands, LANES), jnp.bfloat16),
                pltpu.VMEM((device_total, slots * bands, high // bands, LANES), jnp.bfloat16),
                pltpu.VMEM((device_total // 2, carried, high // bands, LANES), jnp.bfloat16),
                pltpu.VMEM((lat_total // LANES, slot_rows * depth, LANES), jnp.float32),
                pltpu.VMEM((width, width), jnp.float32),
                pltpu.VMEM((pieces, PIECE + 1, month_total), jnp.float32),
                pltpu.VMEM((pieces, PIECE + 1, month_total), jnp.float32),
                pltpu.VMEM((PIECE + 1, month_total), jnp.float32),
                pltpu.VMEM((lat_devices, PIECE + 1, month_total), jnp.float32),
                dma((CHUNKS,)),
                dma((len(phases),)),
                dma((2,)),
                dma((len(phases),)),
                dma((len(phases),)),
                pltpu.SemaphoreType.REGULAR((2,)),
                dma((3,)),
                dma((4,)),
            ],
            compiler_params=pltpu.CompilerParams(
                collective_id=0, has_side_effects=True, vmem_limit_bytes=60 * 1024 * 1024
            ),
        )(fields.reshape(rows * months, lon_count), table, starts, lats)

    return jax.shard_map(
        local, mesh=mesh, in_specs=(P("lat", "tm", None),), out_specs=P("tm", None), check_vma=False
    )
```
